32 devices in a mesh: member: 2 (over x), lon: 8 (over z, y), lat: 2 (over core).
Axes of the slice: x: 2, y: 2, z: 4, core: 2. Of those that a mesh axis runs over, the one named last changes fastest.
Arguments:
- strain_rate: float32 [3, 256, 2160], P(None, 'lon', 'lat'), may hold values from -6 to 6
- stress_start: float32 [3, 256, 2160], P(None, 'lon', 'lat'), may hold values from -3 to 3
- concentration: float32 [256, 2160], P('lon', 'lat'), may hold values from 0.5 to 1
- cell_class: int32 [512, 2160], P(('member', 'lon'), 'lat'), parts along dimension 0, may hold values from 0 to 7
- land_mask: int32 [256, 2160], P('lon', 'lat'), may hold values 0 or 1
- fold_partner: int32 [256], replicated, may hold values from 0 to 255, each once
- kernel_weights: float32 [7, 7], replicated, may hold values from 0.05 to 0.5
Outputs:
- stress_out: float32 [3, 512, 2160], P(None, ('member', 'lon'), 'lat'), parts along dimension 1
- damage_out: float32 [512, 2160], P(('member', 'lon'), 'lat'), parts along dimension 0
- mean_overstress: float32 [6], P('member'), parts along dimension 0
The draws below stay inside these ranges and needn't reach their ends.
There are 2 independent parts, one for each index of `member`. The reference program is written for one: setup_inputs(seed, part) draws one part's arguments, and reference() takes and returns one part's arrays. A program takes and returns all parts, laid end to end along the dimension named above; an argument that names none is the same for every part. Nothing has to cross between parts.
Inputs may be any that keep to these rules, and one draw needn't show every extreme that they name: `fold_partner`: each of the 256 longitude indices appears once.
All inputs are finite; a program needn't handle non-finite values. No bound on the sum of `land_mask` on one device may be relied on, other than what follows from the above.
Results may differ from the reference program's by a relative error of at most 0.0001.
Values sent between devices are 32-bit elements; how exact they have to be, the bound alone decides.
A program may use at most 64 MiB of HBM per device.

```python
import math
import jax
import jax.numpy as jnp

ITERS = 3
KW = 7
NLON = 256
NLAT = 2160


def set_ends(result, key, least, top_value):
    longest = result.shape.index(max(result.shape))
    spots = []
    for shift in (0, 1):
        where = [jax.random.randint(jax.random.fold_in(key, axis), (), 0, length) for axis, length in enumerate(result.shape)]
        where[longest] = (where[longest] + shift) % result.shape[longest]
        spots.append(tuple(where))
    return result.at[spots[0]].set(least).at[spots[1]].set(top_value)


def shard_levels(own_key, extent, shards, low, top_value):
    def one(position, blocks):
        steps = jax.random.uniform(jax.random.fold_in(jax.random.fold_in(own_key, 6), position), (blocks,), jnp.float32, low / len(shards), top_value / len(shards))
        return jnp.repeat(jnp.exp(steps), extent[position] // blocks).reshape((-1,) + (1,) * (len(extent) - position - 1))

    gain = one(*shards[0])
    for cut in shards[1:]:
        gain = gain * one(*cut)
    return gain


def scatter_about(stream_key, extent, scale, most, pieces=(), dtype=jnp.bfloat16):
    gain = shard_levels(stream_key, extent, pieces, -0.22, 0.18) if pieces else 1.0
    values = jax.random.normal(stream_key, extent, jnp.float32) * scale * gain
    return jnp.minimum(jnp.maximum(values, -most), most).astype(dtype)


def setup_inputs(seed: int = 0, part: int = 0) -> dict:
    streams_of = jax.random.split(jax.random.key(seed), 8)
    part_splits = jax.random.split(jax.random.fold_in(streams_of[7], part), 8)
    return {
        "strain_rate": scatter_about(streams_of[0], (3, NLON, NLAT), 1.0, 6.0, ((1, 8), (2, 2)), jnp.float32),
        "stress_start": scatter_about(streams_of[1], (3, NLON, NLAT), 0.5, 3.0, ((1, 8), (2, 2)), jnp.float32),
        "concentration": jnp.clip(0.5 + 0.5 * jax.random.uniform(streams_of[2], (NLON, NLAT), jnp.float32) ** shard_levels(streams_of[2], (NLON, NLAT), ((0, 8), (1, 2)), -0.2, 0.2), 0.5, 1.0),
        "cell_class": set_ends(jax.random.randint(part_splits[3], (NLON, NLAT), 0, 8), jax.random.fold_in(part_splits[3], 1), 0, 7).astype(jnp.int32),
        "land_mask": set_ends((jax.random.randint(streams_of[4], (NLON, NLAT), 0, 4) < 3).astype(jnp.int32), jax.random.fold_in(streams_of[4], 1), 0, 1),
        "fold_partner": jax.random.permutation(streams_of[5], NLON).astype(jnp.int32),
        "kernel_weights": jnp.clip(jnp.exp(jax.random.uniform(streams_of[6], (KW, KW), jnp.float32, math.log(0.05), math.log(0.5))), 0.05, 0.5),
    }


def extend(fields, partner, width):
    top = fields[:, :, -width:]
    north = jnp.take(top, partner, axis=1)[:, :, ::-1]
    south = jnp.zeros_like(north)
    tall = jnp.concatenate([south, fields, north], axis=2)
    return jnp.concatenate([tall[:, -width:], tall, tall[:, :width]], axis=1)

def smooth(padded, weights, ncols, nrows):
    side = weights.shape[0]
    total = jnp.zeros((padded.shape[0], ncols, nrows), jnp.float32)
    for first in range(side):
        for second in range(side):
            total = total + weights[first, second] * padded[:, first:first + ncols, second:second + nrows]
    return total

def reference(strain_rate, stress_start, concentration, cell_class, land_mask, fold_partner, kernel_weights):
    width = kernel_weights.shape[0] // 2
    ocean = land_mask.astype(jnp.float32)
    ncols, nrows = ocean.shape
    denom = smooth(extend(ocean[None], fold_partner, width), kernel_weights, ncols, nrows)[0] + 1.0
    count = jnp.sum(ocean)
    damage = ocean * 0.1 * cell_class.astype(jnp.float32) * concentration
    stress = ocean[None] * stress_start
    base = concentration * jnp.exp(-2.0 * (1.0 - concentration))
    e_one, e_two, e_shear = (strain_rate[0], strain_rate[1], strain_rate[2])
    load = jnp.stack([e_one + e_two / 3.0, e_two + e_one / 3.0, e_shear / (4.0 / 3.0)]) / (8.0 / 9.0)
    means = []
    for step in range(ITERS):
        keep = 1.0 - damage
        theta = 0.5 / (keep * keep)
        elastic = ocean[None] * (stress + (base * keep)[None] * load) / (1.0 + theta)[None]
        half_diff = (elastic[0] - elastic[1]) / 2.0
        tau = jnp.sqrt(half_diff * half_diff + elastic[2] * elastic[2] + 0.25)
        ratio = (tau + 0.7 * (elastic[0] + elastic[1]) / 2.0) / (0.6 * concentration)
        over = jnp.maximum(ratio, 1.0)
        q_part = 1.0 - 1.0 / over
        mean_now = jnp.sum(ocean * (over - 1.0)) / (count + 1.0)
        means.append(mean_now)
        factor = 1.0 / (1.0 + 2.0 * mean_now)
        local_damage = ocean * (damage + factor * keep * q_part)
        local_stress = elastic * (1.0 - factor * q_part)[None]
        fields = jnp.concatenate([local_damage[None], local_stress], axis=0)
        averaged = smooth(extend(fields, fold_partner, width), kernel_weights, ncols, nrows) / denom[None]
        fresh = ocean[None] * (0.5 * fields + 0.5 * averaged)
        damage = fresh[0]
        stress = fresh[1:]
    return (stress, damage, jnp.stack(means).astype(jnp.float32))
```

```python
import functools

import jax
import jax.numpy as jnp
from jax import lax
from jax.experimental import pallas as pl
from jax.experimental.pallas import tpu as pltpu
from jax.sharding import PartitionSpec as P

ITERS = 3
LANES = 128
SUB = 8
MESH = pl.DeviceIdType.MESH
F32 = jnp.float32


def kernel(
    nlon, nlat, nrows, R, L, side,
    w_ref, partner_ref, e_ref, s_ref, conc_ref, class_ref, mask_ref,
    stress_ref, damage_ref, mean_ref,
    Z, Y, X, T, load, base, ocean, rlim, rden, state, C, G, XC, D,
    up_out, down_out, low_in, high_in, ocean_out, ocean_in,
    slab, lat_in, fold_in, stat, stat_in, stage, tops,
    row_send, row_recv, oc_send, oc_recv, lat_send, lat_recv, fold_send, fold_recv, stat_send, stat_recv,
):
    width = side // 2
    n = nlon * nlat
    ncols = R * SUB
    lon, lat = lax.axis_index("lon"), lax.axis_index("lat")
    member = lax.axis_index("member")
    is_last = lat == nlat - 1
    me = lon * nlat + lat
    nb = nrows - (L - LANES)

    def dev(a, b):
        return (member, a, b)

    def peer(d):
        other = lax.rem(me + d, n)
        return dev(other // nlat, lax.rem(other, nlat))

    right, left = lax.rem(lon + 1, nlon), lax.rem(lon + nlon - 1, nlon)
    other_lat = lax.rem(lat + 1, nlat)

    barrier = pltpu.get_barrier_semaphore()

    def greet(d, c):
        pl.semaphore_signal(barrier, inc=1, device_id=peer(d), device_id_type=MESH)
        return c

    lax.fori_loop(1, n, greet, 0)

    sub = lax.broadcasted_iota(jnp.int32, (SUB, L), 0)
    lane = lax.broadcasted_iota(jnp.int32, (SUB, LANES), 1)

    for ref in (load, base, ocean, rlim, state, stage):
        ref[...] = jnp.zeros(ref.shape, F32)
    tiles = L // LANES
    span = [min(LANES, nrows - t * LANES) for t in range(tiles)]
    sources = (
        mask_ref, conc_ref, class_ref, s_ref.at[0], s_ref.at[1], s_ref.at[2], e_ref.at[0], e_ref.at[1], e_ref.at[2]
    )
    for t in range(tiles):
        cut = slice(t * LANES, t * LANES + span[t])
        for k, source in enumerate(sources):
            stage[k, t, :, : span[t]] = source[:, cut].astype(F32)
        for r in range(R):
            oc, conc, grade, s1, s2, s3, one, two, shear = (
                stage[k, t, pl.ds(r, SUB, stride=R), :][:, : span[t]] for k in range(9)
            )
            ocean[r, :, cut] = oc
            base[r, :, cut] = conc * jnp.exp(-2.0 * (1.0 - conc))
            rlim[r, :, cut] = 1.0 / (0.6 * conc)
            state[0, r, :, cut] = oc * 0.1 * grade * conc
            for k, part in enumerate((s1, s2, s3)):
                state[1 + k, r, :, cut] = oc * part
            load[0, r, :, cut] = (one + two / 3.0) / (8.0 / 9.0)
            load[1, r, :, cut] = (two + one / 3.0) / (8.0 / 9.0)
            load[2, r, :, cut] = (shear / (4.0 / 3.0)) / (8.0 / 9.0)
    count = jnp.zeros((1, L), F32)
    for r in range(R):
        Z[8, r] = ocean[r]
        count = count + jnp.sum(ocean[r], axis=0, keepdims=True)
    count = functools.reduce(
        lambda a, b: a + b, [count[:, t * LANES : (t + 1) * LANES] for t in range(L // LANES)]
    )
    ocean_out[...] = jnp.zeros(ocean_out.shape, F32)
    for m in range(width):
        ocean_out[0, m : m + 1, :] = ocean[R - width + m, SUB - 1 : SUB, :]
        ocean_out[1, m : m + 1, :] = ocean[m, 0:1, :]
    slab[...] = jnp.zeros(slab.shape, F32)
    up_out[...] = jnp.zeros(up_out.shape, F32)
    down_out[...] = jnp.zeros(down_out.shape, F32)

    pl.semaphore_wait(barrier, n - 1)

    def ocean_copy(k, to):
        return pltpu.make_async_remote_copy(
            src_ref=ocean_out.at[k], dst_ref=ocean_in.at[k], send_sem=oc_send.at[k],
            recv_sem=oc_recv.at[k], device_id=dev(to, lat), device_id_type=MESH,
        )

    ocean_copy(0, right).start()
    ocean_copy(1, left).start()

    def conv(f, c):
        for r in range(R):
            X[width + r] = Z[f, r]
        for m in range(width):
            X[m] = jnp.where(sub == 0, 0.0, pltpu.roll(Z[f, m + R - width], 1, 0))
            X[R + width + m] = jnp.where(sub == SUB - 1, 0.0, pltpu.roll(Z[f, m], SUB - 1, 0))
        for b in range(side):
            acc = [None] * R
            for p in range(R + 2 * width):
                x = X[p]
                for r in range(R):
                    a = p - r
                    if 0 <= a < side:
                        term = w_ref[a, b] * x
                        acc[r] = term if acc[r] is None else acc[r] + term
            for r in range(R):
                moved = acc[r] if b == width else pltpu.roll(acc[r], (width - b) % L, 1)
                if b == 0:
                    Y[f, r] = moved
                else:
                    Y[f, r] = Y[f, r] + moved
        return c

    def row_correction(halos):
        for r in range(width):
            total = None
            for b in range(side):
                t = None
                for m in range(r, width):
                    d = m - r
                    w = jnp.where(sub < 4, w_ref[d, b], w_ref[side - 1 - d, b])
                    term = w * halos[m]
                    t = term if t is None else t + term
                t = t if b == width else pltpu.roll(t, (width - b) % L, 1)
                total = t if total is None else total + t
            C[r] = total

    def add_rows(f, c):
        for r in range(width):
            Y[f, r] = Y[f, r] + jnp.where(sub == 0, C[r, c : c + 1, :], 0.0)
            Y[f, R - 1 - r] = Y[f, R - 1 - r] + jnp.where(sub == SUB - 1, C[r, 4 + c : 5 + c, :], 0.0)

    def add_columns(f):
        for r in range(R):
            total = None
            for b in range(side):
                t = None
                for a in range(side):
                    term = w_ref[a, b] * XC[r + a]
                    t = term if t is None else t + term
                t = t if b == width else pltpu.roll(t, (width - b) % LANES, 1)
                total = t if total is None else total + t
            Y[f, r, :, L - LANES :] = Y[f, r, :, L - LANES :] + jnp.where(
                (lane >= nb - width) & (lane < nb), total, 0.0
            )
            Y[f, r, :, :LANES] = Y[f, r, :, :LANES] + jnp.where(lane < width, total, 0.0)

    def ghost(at, factor_of):
        for p in range(R + 2 * width):
            north = jnp.where(
                is_last,
                pltpu.roll(factor_of(1, p), (nb - 16 - at) % LANES, 1),
                pltpu.roll(factor_of(0, p), (nb - at) % LANES, 1),
            )
            south = jnp.where(
                lat > 0, pltpu.roll(factor_of(0, p), (LANES - width - 64 - at) % LANES, 1), 0.0
            )
            XC[p] = jnp.where(
                (lane >= nb) & (lane < nb + width), north,
                jnp.where(lane >= LANES - width, south, 0.0),
            )

    def iteration(it, carry):
        excess = jnp.zeros((SUB, L), F32)
        for r in range(R):
            oc = ocean[r]
            damage = state[0, r]
            keep = 1.0 - damage
            theta = 0.5 / (keep * keep)
            scale = oc / (1.0 + theta)
            bk = base[r] * keep
            el = [scale * (state[1 + k, r] + bk * load[k, r]) for k in range(3)]
            half = (el[0] - el[1]) * 0.5
            tau = jnp.sqrt(half * half + el[2] * el[2] + 0.25)
            over = jnp.maximum((tau + 0.35 * (el[0] + el[1])) * rlim[r], 1.0)
            q = oc * (1.0 - 1.0 / over)
            excess = excess + oc * (over - 1.0)
            Z[0, r] = damage
            Z[4, r] = keep * q
            for k in range(3):
                Z[1 + k, r] = el[k]
                Z[5 + k, r] = -(el[k] * q)
            T[r] = q
        for m in range(width):
            hi = R - width + m
            q_row = 4 + m
            for f in range(4):
                at = 4 * m + f
                up_out[it, at // 8, at % 8 : at % 8 + 1, :] = Z[f, hi, SUB - 1 : SUB, :]
                down_out[it, at // 8, at % 8 : at % 8 + 1, :] = Z[f, m, 0:1, :]
            up_out[it, 1, q_row : q_row + 1, :] = T[hi, SUB - 1 : SUB, :]
            down_out[it, 1, q_row : q_row + 1, :] = T[m, 0:1, :]
        up = pltpu.make_async_remote_copy(
            src_ref=up_out.at[it], dst_ref=low_in.at[it], send_sem=row_send.at[it, 0],
            recv_sem=row_recv.at[it, 0], device_id=dev(right, lat), device_id_type=MESH,
        )
        down = pltpu.make_async_remote_copy(
            src_ref=down_out.at[it], dst_ref=high_in.at[it], send_sem=row_send.at[it, 1],
            recv_sem=row_recv.at[it, 1], device_id=dev(left, lat), device_id_type=MESH,
        )
        lines = jnp.sum(excess, axis=0, keepdims=True)
        stat[it, 0:1, :] = functools.reduce(
            lambda a, b: a + b, [lines[:, t * LANES : (t + 1) * LANES] for t in range(L // LANES)]
        )
        stat[it, 1:2, :] = count

        def stat_copy(d):
            return pltpu.make_async_remote_copy(
                src_ref=stat.at[it], dst_ref=stat_in.at[it, d], send_sem=stat_send.at[it, d],
                recv_sem=stat_recv.at[it, d], device_id=peer(d), device_id_type=MESH,
            )

        def start_stat(d, c):
            stat_copy(d).start()
            return c

        lax.fori_loop(1, n, start_stat, 0)
        up.start()
        down.start()

        for r in range(R):
            value = jnp.zeros((SUB, LANES), F32)
            for f in range(9):
                at = 3 * f if f < 4 else (32 + 3 * (f - 4) if f < 8 else 12)
                first = Z[f, r, :, :LANES]
                last = Z[f, r, :, L - LANES :]
                value = jnp.where(
                    (lane >= at) & (lane < at + width), pltpu.roll(first, at, 1), value
                )
                value = jnp.where(
                    (lane >= at + 64) & (lane < at + 64 + width),
                    pltpu.roll(last, (at + 64 + width - nb) % LANES, 1), value,
                )
                for k in range(width):
                    value = jnp.where(
                        lane == at + 16 + k, pltpu.roll(last, (at + 16 + k - (nb - 1 - k)) % LANES, 1), value
                    )
            slab[it, r * SUB : (r + 1) * SUB, :] = value

        def lat_copy(k):
            to = lax.rem(lon + 1 - k + nlon, nlon)
            return pltpu.make_async_remote_copy(
                src_ref=slab.at[it], dst_ref=lat_in.at[it, k], send_sem=lat_send.at[it, k],
                recv_sem=lat_recv.at[it, k], device_id=dev(to, other_lat), device_id_type=MESH,
            )

        def fold_copy(d):
            return pltpu.make_async_remote_copy(
                src_ref=slab.at[it], dst_ref=fold_in.at[it, pl.ds(pl.multiple_of(lon * ncols, SUB), ncols), :],
                send_sem=fold_send.at[it, d], recv_sem=fold_recv.at[it, d],
                device_id=dev(lax.rem(lon + d, nlon), lat), device_id_type=MESH,
            )

        for k in range(3):
            lat_copy(k).start()

        @pl.when(is_last)
        def _():
            def start_fold(d, c):
                fold_copy(d).start()
                return c

            lax.fori_loop(1, nlon, start_fold, 0)
            fold_in[it, pl.ds(pl.multiple_of(lon * ncols, SUB), ncols), :] = slab[it]

        lax.fori_loop(0, jnp.where(it == 0, 9, 8), conv, 0)

        def wait_stat(d, c):
            stat_copy(d).wait()
            return c

        lax.fori_loop(1, n, wait_stat, 0)
        stat_in[it, 0] = stat[it]

        def add_stat(d, total):
            return total + stat_in[it, d]

        total = lax.fori_loop(1, n, add_stat, stat_in[it, 0])
        sums = jnp.sum(total, axis=1, keepdims=True)
        mean = sums[0:1] / (sums[1:2] + 1.0)
        factor = 1.0 / (1.0 + 2.0 * mean)
        mean_ref[pl.ds(it, 1), :] = jnp.broadcast_to(mean, (1, LANES))

        up.wait()
        down.wait()
        for k in range(3):
            lat_copy(k).wait()

        @pl.when(is_last)
        def _():
            def wait_fold(d, c):
                fold_copy(d).wait()
                return c

            lax.fori_loop(1, nlon, wait_fold, 0)

            tops[...] = fold_in[it]

            def pick(i, c):
                where = lax.rem(lon * ncols + i - width + nlon * ncols, nlon * ncols)
                p = partner_ref[where]
                col = lax.rem(p, ncols)
                row = (p // ncols) * ncols + lax.rem(col, R) * SUB + col // R
                D[pl.ds(i, 1), :] = tops[pl.ds(row, 1), :]
                return c

            lax.fori_loop(0, ncols + 2 * width, pick, 0)
            for p in range(R + 2 * width):
                G[1, p] = D[pl.ds(p, SUB, stride=R), :]

        @pl.when(jnp.logical_not(is_last))
        def _():
            for p in range(R + 2 * width):
                G[1, p] = jnp.zeros((SUB, LANES), F32)

        small = lax.broadcasted_iota(jnp.int32, (SUB, LANES), 0)
        for r in range(R):
            G[0, width + r] = lat_in[it, 1, r * SUB : (r + 1) * SUB, :]
        for m in range(width):
            r = m + R - width
            at = slice(r * SUB, (r + 1) * SUB)
            G[0, m] = jnp.where(
                small == 0, pltpu.roll(lat_in[it, 0, at, :], 1, 0), pltpu.roll(lat_in[it, 1, at, :], 1, 0)
            )
            at = slice(m * SUB, (m + 1) * SUB)
            G[0, R + width + m] = jnp.where(
                small == SUB - 1,
                pltpu.roll(lat_in[it, 2, at, :], SUB - 1, 0), pltpu.roll(lat_in[it, 1, at, :], SUB - 1, 0),
            )

        @pl.when(it == 0)
        def _():
            ocean_copy(0, right).wait()
            ocean_copy(1, left).wait()
            row_correction([
                jnp.concatenate([
                    jnp.broadcast_to(ocean_in[0, m : m + 1, :], (4, L)),
                    jnp.broadcast_to(ocean_in[1, width - 1 - m : width - m, :], (4, L)),
                ], axis=0)
                for m in range(width)
            ])
            add_rows(8, 0)
            ghost(12, lambda k, p: G[k, p])
            add_columns(8)
            for r in range(R):
                rden[r] = 1.0 / (Y[8, r] + 1.0)

        head = lax.broadcasted_iota(jnp.int32, (4, L), 0) == 0

        def local_rows(ref, m):
            fq = factor * ref[it, 1, 4 + m : 5 + m, :]
            at = 4 * m
            field = ref[it, at // 8, at % 8 : at % 8 + 4, :]
            return field * (1.0 - fq) + jnp.where(head, fq, 0.0)

        row_correction([
            jnp.concatenate([local_rows(low_in, m), local_rows(high_in, width - 1 - m)], axis=0)
            for m in range(width)
        ])
        for k in range(2):
            for p in range(R + 2 * width):
                g = G[k, p]
                G[k, p] = g + factor * pltpu.roll(g, LANES - 32, 1)
        for f in range(4):
            for r in range(R):
                Y[f, r] = Y[f, r] + factor * Y[4 + f, r]
            add_rows(f, f)
            ghost(3 * f, lambda k, p: G[k, p])
            add_columns(f)
            for r in range(R):
                state[f, r] = (0.5 * ocean[r]) * (Z[f, r] + factor * Z[4 + f, r] + Y[f, r] * rden[r])
        return carry

    lax.fori_loop(0, ITERS, iteration, 0)
    outputs = (damage_ref, stress_ref.at[0], stress_ref.at[1], stress_ref.at[2])
    for t in range(tiles):
        cut = slice(t * LANES, t * LANES + span[t])
        for k, target in enumerate(outputs):
            for r in range(R):
                stage[k, t, pl.ds(r, SUB, stride=R), :] = state[k, r, :, t * LANES : (t + 1) * LANES]
            target[:, cut] = stage[k, t, :, : span[t]]


def shards(nlon, nlat, strain_rate, stress_start, concentration, cell_class, land_mask, fold_partner, kernel_weights):
    ncols, nrows = concentration.shape
    side = kernel_weights.shape[0]
    width = side // 2
    R = ncols // SUB
    L = -(-(nrows + 2 * width) // LANES) * LANES
    n = nlon * nlat
    V = lambda *shape: pltpu.VMEM(shape, F32)
    S = lambda *shape: pltpu.SemaphoreType.DMA(shape)
    planes = R + 2 * width
    stress, damage, mean = pl.pallas_call(
        functools.partial(kernel, nlon, nlat, nrows, R, L, side),
        out_shape=(
            jax.ShapeDtypeStruct((3, ncols, nrows), F32),
            jax.ShapeDtypeStruct((ncols, nrows), F32),
            jax.ShapeDtypeStruct((ITERS, LANES), F32),
        ),
        in_specs=[pl.BlockSpec(memory_space=pltpu.SMEM)] * 2 + [pl.BlockSpec(memory_space=pltpu.VMEM)] * 5,
        out_specs=(pl.BlockSpec(memory_space=pltpu.VMEM),) * 3,
        scratch_shapes=[
            V(9, R, SUB, L), V(9, R, SUB, L), V(planes, SUB, L), V(R, SUB, L),
            V(3, R, SUB, L), V(R, SUB, L), V(R, SUB, L), V(R, SUB, L), V(R, SUB, L), V(4, R, SUB, L),
            V(width, SUB, L), V(2, planes, SUB, LANES), V(planes, SUB, LANES),
            V(-(-(ncols + 2 * width) // SUB) * SUB, LANES),
            V(ITERS, 2, SUB, L), V(ITERS, 2, SUB, L), V(ITERS, 2, SUB, L), V(ITERS, 2, SUB, L),
            V(2, SUB, L), V(2, SUB, L),
            V(ITERS, ncols, LANES), V(ITERS, 3, ncols, LANES), V(ITERS, nlon * ncols, LANES),
            V(ITERS, 2, LANES), V(ITERS, n, 2, LANES), V(9, L // LANES, ncols, LANES), V(nlon * ncols, LANES),
            S(ITERS, 2), S(ITERS, 2), S(2), S(2), S(ITERS, 3), S(ITERS, 3), S(ITERS, nlon), S(ITERS, nlon),
            S(ITERS, n), S(ITERS, n),
        ],
        compiler_params=pltpu.CompilerParams(
            collective_id=0, has_side_effects=True, vmem_limit_bytes=48 * 1024 * 1024
        ),
    )(kernel_weights, fold_partner, strain_rate, stress_start, concentration, cell_class, land_mask)
    return stress, damage, mean[:, 0]


def solution(mesh):
    in_specs = (
        P(None, "lon", "lat"),
        P(None, "lon", "lat"),
        P("lon", "lat"),
        P(("member", "lon"), "lat"),
        P("lon", "lat"),
        P(),
        P(),
    )
    out_specs = (P(None, ("member", "lon"), "lat"), P(("member", "lon"), "lat"), P("member"))
    body = functools.partial(shards, mesh.shape["lon"], mesh.shape["lat"])
    return jax.shard_map(body, mesh=mesh, in_specs=in_specs, out_specs=out_specs, check_vma=False)
```

```python
import functools

import jax
import jax.numpy as jnp
from jax import lax
from jax.experimental import pallas as pl
from jax.experimental.pallas import tpu as pltpu
from jax.sharding import PartitionSpec as P

ITERS = 3
LANES = 128
SUB = 8
MESH = pl.DeviceIdType.MESH
F32 = jnp.float32


def kernel(
    nlon, nlat, nrows, R, L, side,
    w_ref, partner_ref, e_hbm, s_hbm, conc_hbm, class_hbm, mask_hbm,
    stress_ref, damage_ref, mean_ref,
    Z, Y, X, load, base, ocean, rlim, rden, state, C, G, XC, D,
    up_out, down_out, low_in, high_in, ocean_out, ocean_in,
    slab, lat_in, fold_in, stat, stat_in, stage, tops, HQ, HL,
    e_ref, s_ref, conc_ref, class_ref, mask_ref, in_sem,
    row_send, row_recv, oc_send, oc_recv, lat_send, lat_recv, fold_send, fold_recv, stat_send, stat_recv,
):
    width = side // 2
    n = nlon * nlat
    ncols = R * SUB
    lon, lat = lax.axis_index("lon"), lax.axis_index("lat")
    member = lax.axis_index("member")
    is_last = lat == nlat - 1
    me = lon * nlat + lat
    nb = nrows - (L - LANES)

    def dev(a, b):
        return (member, a, b)

    def peer(d):
        other = lax.rem(me + d, n)
        return dev(other // nlat, lax.rem(other, nlat))

    right, left = lax.rem(lon + 1, nlon), lax.rem(lon + nlon - 1, nlon)
    other_lat = lax.rem(lat + 1, nlat)

    loads = [
        pltpu.make_async_copy(a, b, in_sem.at[k])
        for k, (a, b) in enumerate((
            (mask_hbm, mask_ref), (conc_hbm, conc_ref), (class_hbm, class_ref), (s_hbm, s_ref), (e_hbm, e_ref)
        ))
    ]
    for copy in loads:
        copy.start()
    barrier = pltpu.get_barrier_semaphore()

    def greet(d, c):
        pl.semaphore_signal(barrier, inc=1, device_id=peer(d), device_id_type=MESH)
        return c

    lax.fori_loop(1, n, greet, 0)

    sub = lax.broadcasted_iota(jnp.int32, (SUB, L), 0)
    lane = lax.broadcasted_iota(jnp.int32, (SUB, LANES), 1)

    for ref in (load, base, ocean, rlim, state, stage):
        ref[...] = jnp.zeros(ref.shape, F32)
    slab[...] = jnp.zeros(slab.shape, F32)
    ocean_out[...] = jnp.zeros(ocean_out.shape, F32)
    HQ[...] = jnp.zeros(HQ.shape, F32)
    HL[...] = jnp.zeros(HL.shape, F32)
    for copy in loads:
        copy.wait()
    tiles = L // LANES
    span = [min(LANES, nrows - t * LANES) for t in range(tiles)]
    sources = (
        mask_ref, conc_ref, class_ref, s_ref.at[0], s_ref.at[1], s_ref.at[2], e_ref.at[0], e_ref.at[1], e_ref.at[2]
    )
    for t in range(tiles):
        cut = slice(t * LANES, t * LANES + span[t])
        for k, source in enumerate(sources):
            stage[k, t, :, : span[t]] = source[:, cut].astype(F32)
        for r in range(R):
            oc, conc, grade, s1, s2, s3, one, two, shear = (
                stage[k, t, pl.ds(r, SUB, stride=R), :][:, : span[t]] for k in range(9)
            )
            ocean[r, :, cut] = oc
            base[r, :, cut] = conc * jnp.exp(-2.0 * (1.0 - conc))
            rlim[r, :, cut] = 1.0 / (0.6 * conc)
            state[0, r, :, cut] = oc * 0.1 * grade * conc
            for k, part in enumerate((s1, s2, s3)):
                state[1 + k, r, :, cut] = oc * part
            load[0, r, :, cut] = (one + two / 3.0) / (8.0 / 9.0)
            load[1, r, :, cut] = (two + one / 3.0) / (8.0 / 9.0)
            load[2, r, :, cut] = (shear / (4.0 / 3.0)) / (8.0 / 9.0)
    count = jnp.zeros((1, L), F32)
    for r in range(R):
        Z[8, r] = ocean[r]
        count = count + jnp.sum(ocean[r], axis=0, keepdims=True)
    count = functools.reduce(
        lambda a, b: a + b, [count[:, t * LANES : (t + 1) * LANES] for t in range(L // LANES)]
    )
    for m in range(width):
        ocean_out[0, 4 + m : 5 + m, :] = rlim[R - width + m, SUB - 1 : SUB, :]
        ocean_out[1, 4 + m : 5 + m, :] = rlim[m, 0:1, :]
        ocean_out[0, m : m + 1, :] = ocean[R - width + m, SUB - 1 : SUB, :]
        ocean_out[1, m : m + 1, :] = ocean[m, 0:1, :]

    pl.semaphore_wait(barrier, n - 1)

    def ocean_copy(k, to):
        return pltpu.make_async_remote_copy(
            src_ref=ocean_out.at[k], dst_ref=ocean_in.at[k], send_sem=oc_send.at[k],
            recv_sem=oc_recv.at[k], device_id=dev(to, lat), device_id_type=MESH,
        )

    ocean_copy(0, right).start()
    ocean_copy(1, left).start()

    def conv(f, c):
        for r in range(R):
            X[width + r] = Z[f, r]
        for m in range(width):
            X[m] = jnp.where(sub == 0, 0.0, pltpu.roll(Z[f, m + R - width], 1, 0))
            X[R + width + m] = jnp.where(sub == SUB - 1, 0.0, pltpu.roll(Z[f, m], SUB - 1, 0))
        for b in range(side):
            acc = [None] * R
            for p in range(R + 2 * width):
                x = X[p]
                for r in range(R):
                    a = p - r
                    if 0 <= a < side:
                        term = w_ref[a, b] * x
                        acc[r] = term if acc[r] is None else acc[r] + term
            for r in range(R):
                moved = acc[r] if b == width else pltpu.roll(acc[r], (width - b) % L, 1)
                if b == 0:
                    Y[f, r] = moved
                else:
                    Y[f, r] = Y[f, r] + moved
        return c

    def row_correction(halos):
        for r in range(width):
            total = None
            for b in range(side):
                t = None
                for m in range(r, width):
                    d = m - r
                    w = jnp.where(sub < 4, w_ref[d, b], w_ref[side - 1 - d, b])
                    term = w * halos[m]
                    t = term if t is None else t + term
                t = t if b == width else pltpu.roll(t, (width - b) % L, 1)
                total = t if total is None else total + t
            C[r] = total

    def add_rows(f, c):
        for r in range(width):
            Y[f, r] = Y[f, r] + jnp.where(sub == 0, C[r, c : c + 1, :], 0.0)
            Y[f, R - 1 - r] = Y[f, R - 1 - r] + jnp.where(sub == SUB - 1, C[r, 4 + c : 5 + c, :], 0.0)

    def add_columns(f):
        for r in range(R):
            total = None
            for b in range(side):
                t = None
                for a in range(side):
                    term = w_ref[a, b] * XC[r + a]
                    t = term if t is None else t + term
                t = t if b == width else pltpu.roll(t, (width - b) % LANES, 1)
                total = t if total is None else total + t
            Y[f, r, :, L - LANES :] = Y[f, r, :, L - LANES :] + jnp.where(
                (lane >= nb - width) & (lane < nb), total, 0.0
            )
            Y[f, r, :, :LANES] = Y[f, r, :, :LANES] + jnp.where(lane < width, total, 0.0)

    def ghost(at):
        for p in range(R + 2 * width):
            north = pltpu.roll(G[1, p], (nb - at) % LANES, 1)
            south = jnp.where(lat > 0, pltpu.roll(G[0, p], (LANES - width - at) % LANES, 1), 0.0)
            XC[p] = jnp.where(
                (lane >= nb) & (lane < nb + width), north,
                jnp.where(lane >= LANES - width, south, 0.0),
            )

    def iteration(it, carry):
        excess = jnp.zeros((SUB, L), F32)
        for r in range(R):
            oc = ocean[r]
            damage = state[0, r]
            keep = 1.0 - damage
            theta = 0.5 / (keep * keep)
            scale = oc / (1.0 + theta)
            bk = base[r] * keep
            el = [scale * (state[1 + k, r] + bk * load[k, r]) for k in range(3)]
            half = (el[0] - el[1]) * 0.5
            tau = jnp.sqrt(half * half + el[2] * el[2] + 0.25)
            over = jnp.maximum((tau + 0.35 * (el[0] + el[1])) * rlim[r], 1.0)
            q = oc * (1.0 - 1.0 / over)
            excess = excess + oc * (over - 1.0)
            Z[0, r] = damage
            Z[4, r] = keep * q
            for k in range(3):
                Z[1 + k, r] = el[k]
                Z[5 + k, r] = -(el[k] * q)
        for m in range(width):
            hi = R - width + m
            for f in range(4):
                up_out[it, m, f : f + 1, :] = Z[f, hi, SUB - 1 : SUB, :]
                down_out[it, m, f : f + 1, :] = Z[f, m, 0:1, :]
        up = pltpu.make_async_remote_copy(
            src_ref=up_out.at[it], dst_ref=low_in.at[it], send_sem=row_send.at[it, 0],
            recv_sem=row_recv.at[it, 0], device_id=dev(right, lat), device_id_type=MESH,
        )
        down = pltpu.make_async_remote_copy(
            src_ref=down_out.at[it], dst_ref=high_in.at[it], send_sem=row_send.at[it, 1],
            recv_sem=row_recv.at[it, 1], device_id=dev(left, lat), device_id_type=MESH,
        )
        lines = jnp.sum(excess, axis=0, keepdims=True)
        stat[it, 0:1, :] = functools.reduce(
            lambda a, b: a + b, [lines[:, t * LANES : (t + 1) * LANES] for t in range(L // LANES)]
        )
        stat[it, 1:2, :] = count

        def stat_copy(d):
            return pltpu.make_async_remote_copy(
                src_ref=stat.at[it], dst_ref=stat_in.at[it, d], send_sem=stat_send.at[it, d],
                recv_sem=stat_recv.at[it, d], device_id=peer(d), device_id_type=MESH,
            )

        def start_stat(d, c):
            stat_copy(d).start()
            return c

        lax.fori_loop(1, n, start_stat, 0)
        up.start()
        down.start()

        edge = jnp.zeros((SUB, LANES), F32)
        top = jnp.zeros((SUB, LANES), F32)
        for r in range(R):
            for f in range(9):
                at = 32 * r + (3 * f if f < 4 else (16 + 3 * (f - 4) if f < 8 else 12))
                first = Z[f, r, :, :LANES]
                last = Z[f, r, :, L - LANES :]
                both = jnp.where(
                    is_last, pltpu.roll(first, at, 1), pltpu.roll(last, (at + width - nb) % LANES, 1)
                )
                edge = jnp.where((lane >= at) & (lane < at + width), both, edge)
                for k in range(width):
                    top = jnp.where(lane == at + k, pltpu.roll(last, (at + k - (nb - 1 - k)) % LANES, 1), top)
        slab[it, 0] = edge
        slab[it, 1] = top

        def lat_copy(k):
            to = lax.rem(lon + 1 - k + nlon, nlon)
            return pltpu.make_async_remote_copy(
                src_ref=slab.at[it, 0], dst_ref=lat_in.at[it, k], send_sem=lat_send.at[it, k],
                recv_sem=lat_recv.at[it, k], device_id=dev(to, other_lat), device_id_type=MESH,
            )

        def fold_copy(d):
            return pltpu.make_async_remote_copy(
                src_ref=slab.at[it, 1], dst_ref=fold_in.at[it, lon],
                send_sem=fold_send.at[it, d], recv_sem=fold_recv.at[it, d],
                device_id=dev(lax.rem(lon + d, nlon), lat), device_id_type=MESH,
            )

        for k in range(3):
            lat_copy(k).start()

        @pl.when(is_last)
        def _():
            def start_fold(d, c):
                fold_copy(d).start()
                return c

            lax.fori_loop(1, nlon, start_fold, 0)
            fold_in[it, lon] = slab[it, 1]

        lax.fori_loop(0, jnp.where(it == 0, 9, 8), conv, 0)

        def wait_stat(d, c):
            stat_copy(d).wait()
            return c

        lax.fori_loop(1, n, wait_stat, 0)
        stat_in[it, 0] = stat[it]

        def add_stat(d, total):
            return total + stat_in[it, d]

        total = lax.fori_loop(1, n, add_stat, stat_in[it, 0])
        sums = jnp.sum(total, axis=1, keepdims=True)
        mean = sums[0:1] / (sums[1:2] + 1.0)
        factor = 1.0 / (1.0 + 2.0 * mean)
        mean_ref[pl.ds(it, 1), :] = jnp.broadcast_to(mean, (1, LANES))

        up.wait()
        down.wait()
        for k in range(3):
            lat_copy(k).wait()

        @pl.when(is_last)
        def _():
            def wait_fold(d, c):
                fold_copy(d).wait()
                return c

            lax.fori_loop(1, nlon, wait_fold, 0)

            def spread(k, c):
                tile = fold_in[it, k]
                for r in range(R):
                    tops[k, r] = tile if r == 0 else pltpu.roll(tile, LANES - 32 * r, 1)
                return c

            lax.fori_loop(0, nlon, spread, 0)

            def pick(i, c):
                where = lax.rem(lon * ncols + i - width + nlon * ncols, nlon * ncols)
                p = partner_ref[where]
                col = lax.rem(p, ncols)
                D[pl.ds(i, 1), :] = tops[p // ncols, lax.rem(col, R), pl.ds(col // R, 1), :]
                return c

            lax.fori_loop(0, ncols + 2 * width, pick, 0)
            for p in range(R + 2 * width):
                G[1, p] = D[pl.ds(p, SUB, stride=R), :]

        @pl.when(jnp.logical_not(is_last))
        def _():
            for p in range(R + 2 * width):
                G[1, p] = jnp.zeros((SUB, LANES), F32)

        small = lax.broadcasted_iota(jnp.int32, (SUB, LANES), 0)
        def piece(k, r):
            return lat_in[it, k] if r == 0 else pltpu.roll(lat_in[it, k], LANES - 32 * r, 1)

        own = [piece(1, r) for r in range(R)]
        for r in range(R):
            G[0, width + r] = own[r]
        for m in range(width):
            r = m + R - width
            G[0, m] = jnp.where(small == 0, pltpu.roll(piece(0, r), 1, 0), pltpu.roll(own[r], 1, 0))
            G[0, R + width + m] = jnp.where(
                small == SUB - 1, pltpu.roll(piece(2, m), SUB - 1, 0), pltpu.roll(own[m], SUB - 1, 0)
            )
        for p in range(R + 2 * width):
            G[1, p] = jnp.where(is_last, G[1, p], G[0, p])

        @pl.when(it == 0)
        def _():
            ocean_copy(0, right).wait()
            ocean_copy(1, left).wait()
            for k in range(2):
                for m in range(width):
                    HL[k, m : m + 1, :] = ocean_in[0, 4 * k + m : 4 * k + m + 1, :]
                    HL[k, 4 + m : 5 + m, :] = ocean_in[1, 4 * k + m : 4 * k + m + 1, :]
            row_correction([
                jnp.concatenate([
                    jnp.broadcast_to(ocean_in[0, m : m + 1, :], (4, L)),
                    jnp.broadcast_to(ocean_in[1, width - 1 - m : width - m, :], (4, L)),
                ], axis=0)
                for m in range(width)
            ])
            add_rows(8, 0)
            ghost(12)
            add_columns(8)
            for r in range(R):
                rden[r] = 1.0 / (Y[8, r] + 1.0)

        head = lax.broadcasted_iota(jnp.int32, (4, L), 0) == 0

        for k in range(3):
            for m in range(width):
                HQ[k, m : m + 1, :] = low_in[it, m, 1 + k : 2 + k, :]
                HQ[k, 4 + m : 5 + m, :] = high_in[it, m, 1 + k : 2 + k, :]
        half = (HQ[0] - HQ[1]) * 0.5
        tau = jnp.sqrt(half * half + HQ[2] * HQ[2] + 0.25)
        over = jnp.maximum((tau + 0.35 * (HQ[0] + HQ[1])) * HL[1], 1.0)
        HQ[3] = factor * (HL[0] * (1.0 - 1.0 / over))

        def local_rows(ref, side_at, m):
            fq = HQ[3, side_at + m : side_at + m + 1, :]
            return ref[it, m] * (1.0 - fq) + jnp.where(head, fq, 0.0)

        row_correction([
            jnp.concatenate([local_rows(low_in, 0, m), local_rows(high_in, 4, width - 1 - m)], axis=0)
            for m in range(width)
        ])
        for k in range(2):
            for p in range(R + 2 * width):
                g = G[k, p]
                G[k, p] = g + factor * pltpu.roll(g, LANES - 16, 1)
        for f in range(4):
            for r in range(R):
                Y[f, r] = Y[f, r] + factor * Y[4 + f, r]
            add_rows(f, f)
            ghost(3 * f)
            add_columns(f)
            for r in range(R):
                state[f, r] = (0.5 * ocean[r]) * (Z[f, r] + factor * Z[4 + f, r] + Y[f, r] * rden[r])
        return carry

    lax.fori_loop(0, ITERS, iteration, 0)
    outputs = (damage_ref, stress_ref.at[0], stress_ref.at[1], stress_ref.at[2])
    for t in range(tiles):
        cut = slice(t * LANES, t * LANES + span[t])
        for k, target in enumerate(outputs):
            for r in range(R):
                stage[k, t, pl.ds(r, SUB, stride=R), :] = state[k, r, :, t * LANES : (t + 1) * LANES]
            target[:, cut] = stage[k, t, :, : span[t]]


def shards(nlon, nlat, strain_rate, stress_start, concentration, cell_class, land_mask, fold_partner, kernel_weights):
    ncols, nrows = concentration.shape
    side = kernel_weights.shape[0]
    width = side // 2
    R = ncols // SUB
    L = -(-(nrows + 2 * width) // LANES) * LANES
    n = nlon * nlat
    V = lambda *shape: pltpu.VMEM(shape, F32)
    S = lambda *shape: pltpu.SemaphoreType.DMA(shape)
    planes = R + 2 * width
    stress, damage, mean = pl.pallas_call(
        functools.partial(kernel, nlon, nlat, nrows, R, L, side),
        out_shape=(
            jax.ShapeDtypeStruct((3, ncols, nrows), F32),
            jax.ShapeDtypeStruct((ncols, nrows), F32),
            jax.ShapeDtypeStruct((ITERS, LANES), F32),
        ),
        in_specs=[pl.BlockSpec(memory_space=pltpu.SMEM)] * 2 + [pl.BlockSpec(memory_space=pltpu.HBM)] * 5,
        out_specs=(pl.BlockSpec(memory_space=pltpu.VMEM),) * 3,
        scratch_shapes=[
            V(9, R, SUB, L), V(9, R, SUB, L), V(planes, SUB, L),
            V(3, R, SUB, L), V(R, SUB, L), V(R, SUB, L), V(R, SUB, L), V(R, SUB, L), V(4, R, SUB, L),
            V(width, SUB, L), V(2, planes, SUB, LANES), V(planes, SUB, LANES),
            V(-(-(ncols + 2 * width) // SUB) * SUB, LANES),
            V(ITERS, width, 4, L), V(ITERS, width, 4, L), V(ITERS, width, 4, L), V(ITERS, width, 4, L),
            V(2, SUB, L), V(2, SUB, L),
            V(ITERS, 2, SUB, LANES), V(ITERS, 3, SUB, LANES), V(ITERS, nlon, SUB, LANES),
            V(ITERS, 2, LANES), V(ITERS, n, 2, LANES), V(9, L // LANES, ncols, LANES), V(nlon, R, SUB, LANES),
            V(4, SUB, L), V(2, SUB, L), V(3, ncols, nrows), V(3, ncols, nrows), V(ncols, nrows),
            pltpu.VMEM((ncols, nrows), jnp.int32), pltpu.VMEM((ncols, nrows), jnp.int32), S(5),
            S(ITERS, 2), S(ITERS, 2), S(2), S(2), S(ITERS, 3), S(ITERS, 3), S(ITERS, nlon), S(ITERS, nlon),
            S(ITERS, n), S(ITERS, n),
        ],
        compiler_params=pltpu.CompilerParams(
            collective_id=0, has_side_effects=True, vmem_limit_bytes=48 * 1024 * 1024
        ),
    )(kernel_weights, fold_partner, strain_rate, stress_start, concentration, cell_class, land_mask)
    return stress, damage, mean[:, 0]


def solution(mesh):
    in_specs = (
        P(None, "lon", "lat"),
        P(None, "lon", "lat"),
        P("lon", "lat"),
        P(("member", "lon"), "lat"),
        P("lon", "lat"),
        P(),
        P(),
    )
    out_specs = (P(None, ("member", "lon"), "lat"), P(("member", "lon"), "lat"), P("member"))
    body = functools.partial(shards, mesh.shape["lon"], mesh.shape["lat"])
    return jax.shard_map(body, mesh=mesh, in_specs=in_specs, out_specs=out_specs, check_vma=False)
```

```python
import functools

import jax
import jax.numpy as jnp
from jax import lax
from jax.experimental import pallas as pl
from jax.experimental.pallas import tpu as pltpu
from jax.sharding import PartitionSpec as P

ITERS = 3
LANES = 128
SUB = 8
MESH = pl.DeviceIdType.MESH
F32 = jnp.float32


def kernel(
    nlon, nlat, nrows, R, L, side,
    w_ref, partner_ref, e_hbm, s_hbm, conc_hbm, class_hbm, mask_hbm,
    stress_ref, damage_ref, mean_ref,
    Z, Y, X, load, base, ocean, rlim, rden, state, C, G, XC, D,
    up_out, down_out, low_in, high_in, ocean_out, ocean_in,
    slab, lat_in, fold_in, stat, stat_in, stage, tops, HQ, HL,
    e_ref, s_ref, conc_ref, class_ref, mask_ref, in_sem,
    row_send, row_recv, oc_send, oc_recv, lat_send, lat_recv, fold_send, fold_recv, stat_send, stat_recv,
):
    width = side // 2
    n = nlon * nlat
    ncols = R * SUB
    lon, lat = lax.axis_index("lon"), lax.axis_index("lat")
    member = lax.axis_index("member")
    is_last = lat == nlat - 1
    me = lon * nlat + lat
    nb = nrows - (L - LANES)

    def dev(a, b):
        return (member, a, b)

    def peer(d):
        other = lax.rem(me + d, n)
        return dev(other // nlat, lax.rem(other, nlat))

    right, left = lax.rem(lon + 1, nlon), lax.rem(lon + nlon - 1, nlon)
    other_lat = lax.rem(lat + 1, nlat)

    loads = [
        pltpu.make_async_copy(a, b, in_sem.at[k])
        for k, (a, b) in enumerate((
            (mask_hbm, mask_ref), (conc_hbm, conc_ref), (class_hbm, class_ref), (s_hbm, s_ref), (e_hbm, e_ref)
        ))
    ]
    for copy in loads:
        copy.start()
    barrier = pltpu.get_barrier_semaphore()

    def greet(d, c):
        pl.semaphore_signal(barrier, inc=1, device_id=peer(d), device_id_type=MESH)
        return c

    lax.fori_loop(1, n, greet, 0)

    sub = lax.broadcasted_iota(jnp.int32, (SUB, L), 0)
    lane = lax.broadcasted_iota(jnp.int32, (SUB, LANES), 1)

    for ref in (load, base, ocean, rlim, state, stage):
        ref[...] = jnp.zeros(ref.shape, F32)
    slab[...] = jnp.zeros(slab.shape, F32)
    ocean_out[...] = jnp.zeros(ocean_out.shape, F32)
    HQ[...] = jnp.zeros(HQ.shape, F32)
    HL[...] = jnp.zeros(HL.shape, F32)
    for copy in loads:
        copy.wait()
    tiles = L // LANES
    span = [min(LANES, nrows - t * LANES) for t in range(tiles)]
    sources = (
        mask_ref, conc_ref, class_ref, s_ref.at[0], s_ref.at[1], s_ref.at[2], e_ref.at[0], e_ref.at[1], e_ref.at[2]
    )
    for t in range(tiles):
        cut = slice(t * LANES, t * LANES + span[t])
        for k, source in enumerate(sources):
            stage[k, t, :, : span[t]] = source[:, cut].astype(F32)
        for r in range(R):
            oc, conc, grade, s1, s2, s3, one, two, shear = (
                stage[k, t, pl.ds(r, SUB, stride=R), :][:, : span[t]] for k in range(9)
            )
            ocean[r, :, cut] = oc
            base[r, :, cut] = conc * jnp.exp(-2.0 * (1.0 - conc))
            rlim[r, :, cut] = 1.0 / (0.6 * conc)
            state[0, r, :, cut] = oc * 0.1 * grade * conc
            for k, part in enumerate((s1, s2, s3)):
                state[1 + k, r, :, cut] = oc * part
            load[0, r, :, cut] = (one + two / 3.0) / (8.0 / 9.0)
            load[1, r, :, cut] = (two + one / 3.0) / (8.0 / 9.0)
            load[2, r, :, cut] = (shear / (4.0 / 3.0)) / (8.0 / 9.0)
    count = jnp.zeros((1, L), F32)
    for r in range(R):
        Z[8, r] = ocean[r]
        count = count + jnp.sum(ocean[r], axis=0, keepdims=True)
    count = functools.reduce(
        lambda a, b: a + b, [count[:, t * LANES : (t + 1) * LANES] for t in range(L // LANES)]
    )
    for m in range(width):
        ocean_out[0, 4 + m : 5 + m, :] = rlim[R - width + m, SUB - 1 : SUB, :]
        ocean_out[1, 4 + m : 5 + m, :] = rlim[m, 0:1, :]
        ocean_out[0, m : m + 1, :] = ocean[R - width + m, SUB - 1 : SUB, :]
        ocean_out[1, m : m + 1, :] = ocean[m, 0:1, :]

    pl.semaphore_wait(barrier, n - 1)

    def ocean_copy(k, to):
        return pltpu.make_async_remote_copy(
            src_ref=ocean_out.at[k], dst_ref=ocean_in.at[k], send_sem=oc_send.at[k],
            recv_sem=oc_recv.at[k], device_id=dev(to, lat), device_id_type=MESH,
        )

    ocean_copy(0, right).start()
    ocean_copy(1, left).start()

    def conv(f, c):
        for r in range(R):
            X[width + r] = Z[f, r]
        for m in range(width):
            X[m] = jnp.where(sub == 0, 0.0, pltpu.roll(Z[f, m + R - width], 1, 0))
            X[R + width + m] = jnp.where(sub == SUB - 1, 0.0, pltpu.roll(Z[f, m], SUB - 1, 0))
        for b in range(side):
            acc = [None] * R
            for p in range(R + 2 * width):
                x = X[p]
                for r in range(R):
                    a = p - r
                    if 0 <= a < side:
                        term = w_ref[a, b] * x
                        acc[r] = term if acc[r] is None else acc[r] + term
            for r in range(R):
                moved = acc[r] if b == width else pltpu.roll(acc[r], (width - b) % L, 1)
                if b == 0:
                    Y[f, r] = moved
                else:
                    Y[f, r] = Y[f, r] + moved
        return c

    def row_correction(halos):
        for r in range(width):
            total = None
            for b in range(side):
                t = None
                for m in range(r, width):
                    d = m - r
                    w = jnp.where(sub < 4, w_ref[d, b], w_ref[side - 1 - d, b])
                    term = w * halos[m]
                    t = term if t is None else t + term
                t = t if b == width else pltpu.roll(t, (width - b) % L, 1)
                total = t if total is None else total + t
            C[r] = total

    def add_rows(f, c):
        for r in range(width):
            Y[f, r] = Y[f, r] + jnp.where(sub == 0, C[r, c : c + 1, :], 0.0)
            Y[f, R - 1 - r] = Y[f, R - 1 - r] + jnp.where(sub == SUB - 1, C[r, 4 + c : 5 + c, :], 0.0)

    def add_columns(f):
        for r in range(R):
            total = None
            for b in range(side):
                t = None
                for a in range(side):
                    term = w_ref[a, b] * XC[r + a]
                    t = term if t is None else t + term
                t = t if b == width else pltpu.roll(t, (width - b) % LANES, 1)
                total = t if total is None else total + t
            Y[f, r, :, L - LANES :] = Y[f, r, :, L - LANES :] + jnp.where(
                (lane >= nb - width) & (lane < nb), total, 0.0
            )
            Y[f, r, :, :LANES] = Y[f, r, :, :LANES] + jnp.where(lane < width, total, 0.0)

    def ghost(at):
        for p in range(R + 2 * width):
            north = pltpu.roll(G[1, p], (nb - at) % LANES, 1)
            south = jnp.where(lat > 0, pltpu.roll(G[0, p], (LANES - width - at) % LANES, 1), 0.0)
            XC[p] = jnp.where(
                (lane >= nb) & (lane < nb + width), north,
                jnp.where(lane >= LANES - width, south, 0.0),
            )

    def iteration(it, carry):
        excess = jnp.zeros((SUB, L), F32)
        for r in range(R):
            oc = ocean[r]
            damage = state[0, r]
            keep = 1.0 - damage
            theta = 0.5 / (keep * keep)
            scale = oc / (1.0 + theta)
            bk = base[r] * keep
            el = [scale * (state[1 + k, r] + bk * load[k, r]) for k in range(3)]
            half = (el[0] - el[1]) * 0.5
            tau = jnp.sqrt(half * half + el[2] * el[2] + 0.25)
            over = jnp.maximum((tau + 0.35 * (el[0] + el[1])) * rlim[r], 1.0)
            q = oc * (1.0 - 1.0 / over)
            excess = excess + oc * (over - 1.0)
            Z[0, r] = damage
            Z[4, r] = keep * q
            for k in range(3):
                Z[1 + k, r] = el[k]
                Z[5 + k, r] = -(el[k] * q)
        for m in range(width):
            hi = R - width + m
            for f in range(4):
                up_out[it, m, f : f + 1, :] = Z[f, hi, SUB - 1 : SUB, :]
                down_out[it, m, f : f + 1, :] = Z[f, m, 0:1, :]
        up = pltpu.make_async_remote_copy(
            src_ref=up_out.at[it], dst_ref=low_in.at[it], send_sem=row_send.at[it, 0],
            recv_sem=row_recv.at[it, 0], device_id=dev(right, lat), device_id_type=MESH,
        )
        down = pltpu.make_async_remote_copy(
            src_ref=down_out.at[it], dst_ref=high_in.at[it], send_sem=row_send.at[it, 1],
            recv_sem=row_recv.at[it, 1], device_id=dev(left, lat), device_id_type=MESH,
        )
        lines = jnp.sum(excess, axis=0, keepdims=True)
        stat[it, 0:1, :] = functools.reduce(
            lambda a, b: a + b, [lines[:, t * LANES : (t + 1) * LANES] for t in range(L // LANES)]
        )
        stat[it, 1:2, :] = count

        def stat_copy(d):
            return pltpu.make_async_remote_copy(
                src_ref=stat.at[it], dst_ref=stat_in.at[it, d], send_sem=stat_send.at[it, d],
                recv_sem=stat_recv.at[it, d], device_id=peer(d), device_id_type=MESH,
            )

        def start_stat(d, c):
            stat_copy(d).start()
            return c

        lax.fori_loop(1, n, start_stat, 0)
        up.start()
        down.start()

        edge = jnp.zeros((SUB, LANES), F32)
        top = jnp.zeros((SUB, LANES), F32)
        for r in range(R):
            for f in range(9):
                at = 32 * r + (3 * f if f < 4 else (16 + 3 * (f - 4) if f < 8 else 12))
                first = Z[f, r, :, :LANES]
                last = Z[f, r, :, L - LANES :]
                both = jnp.where(
                    is_last, pltpu.roll(first, at, 1), pltpu.roll(last, (at + width - nb) % LANES, 1)
                )
                edge = jnp.where((lane >= at) & (lane < at + width), both, edge)
                for k in range(width):
                    top = jnp.where(lane == at + k, pltpu.roll(last, (at + k - (nb - 1 - k)) % LANES, 1), top)
        slab[it, 0] = edge
        slab[it, 1] = top

        def lat_copy(k):
            to = lax.rem(lon + 1 - k + nlon, nlon)
            return pltpu.make_async_remote_copy(
                src_ref=slab.at[it, 0], dst_ref=lat_in.at[it, k], send_sem=lat_send.at[it, k],
                recv_sem=lat_recv.at[it, k], device_id=dev(to, other_lat), device_id_type=MESH,
            )

        def fold_copy(d):
            return pltpu.make_async_remote_copy(
                src_ref=slab.at[it, 1], dst_ref=fold_in.at[it, lon],
                send_sem=fold_send.at[it, d], recv_sem=fold_recv.at[it, d],
                device_id=dev(lax.rem(lon + d, nlon), lat), device_id_type=MESH,
            )

        for k in range(3):
            lat_copy(k).start()

        @pl.when(is_last)
        def _():
            def start_fold(d, c):
                fold_copy(d).start()
                return c

            lax.fori_loop(1, nlon, start_fold, 0)
            fold_in[it, lon] = slab[it, 1]

        lax.fori_loop(0, jnp.where(it == 0, 9, 8), conv, 0)

        def wait_stat(d, c):
            stat_copy(d).wait()
            return c

        lax.fori_loop(1, n, wait_stat, 0)
        stat_in[it, 0] = stat[it]

        def add_stat(d, total):
            return total + stat_in[it, d]

        total = lax.fori_loop(1, n, add_stat, stat_in[it, 0])
        sums = jnp.sum(total, axis=1, keepdims=True)
        mean = sums[0:1] / (sums[1:2] + 1.0)
        factor = 1.0 / (1.0 + 2.0 * mean)
        mean_ref[pl.ds(it, 1), :] = jnp.broadcast_to(mean, (1, LANES))

        for f in range(4):
            for r in range(R):
                Y[f, r] = Y[f, r] + factor * Y[4 + f, r]
                Z[f, r] = Z[f, r] + factor * Z[4 + f, r]

        up.wait()
        down.wait()
        for k in range(3):
            lat_copy(k).wait()

        @pl.when(is_last)
        def _():
            def wait_fold(d, c):
                fold_copy(d).wait()
                return c

            lax.fori_loop(1, nlon, wait_fold, 0)

            def spread(k, c):
                tile = fold_in[it, k]
                for r in range(R):
                    tops[k, r] = tile if r == 0 else pltpu.roll(tile, LANES - 32 * r, 1)
                return c

            lax.fori_loop(0, nlon, spread, 0)

            def pick(i, c):
                where = lax.rem(lon * ncols + i - width + nlon * ncols, nlon * ncols)
                p = partner_ref[where]
                col = lax.rem(p, ncols)
                D[pl.ds(i, 1), :] = tops[p // ncols, lax.rem(col, R), pl.ds(col // R, 1), :]
                return c

            lax.fori_loop(0, ncols + 2 * width, pick, 0)
            for p in range(R + 2 * width):
                G[1, p] = D[pl.ds(p, SUB, stride=R), :]

        @pl.when(jnp.logical_not(is_last))
        def _():
            for p in range(R + 2 * width):
                G[1, p] = jnp.zeros((SUB, LANES), F32)

        small = lax.broadcasted_iota(jnp.int32, (SUB, LANES), 0)
        def piece(k, r):
            return lat_in[it, k] if r == 0 else pltpu.roll(lat_in[it, k], LANES - 32 * r, 1)

        own = [piece(1, r) for r in range(R)]
        for r in range(R):
            G[0, width + r] = own[r]
        for m in range(width):
            r = m + R - width
            G[0, m] = jnp.where(small == 0, pltpu.roll(piece(0, r), 1, 0), pltpu.roll(own[r], 1, 0))
            G[0, R + width + m] = jnp.where(
                small == SUB - 1, pltpu.roll(piece(2, m), SUB - 1, 0), pltpu.roll(own[m], SUB - 1, 0)
            )
        for p in range(R + 2 * width):
            G[1, p] = jnp.where(is_last, G[1, p], G[0, p])

        @pl.when(it == 0)
        def _():
            ocean_copy(0, right).wait()
            ocean_copy(1, left).wait()
            for k in range(2):
                for m in range(width):
                    HL[k, m : m + 1, :] = ocean_in[0, 4 * k + m : 4 * k + m + 1, :]
                    HL[k, 4 + m : 5 + m, :] = ocean_in[1, 4 * k + m : 4 * k + m + 1, :]
            row_correction([
                jnp.concatenate([
                    jnp.broadcast_to(ocean_in[0, m : m + 1, :], (4, L)),
                    jnp.broadcast_to(ocean_in[1, width - 1 - m : width - m, :], (4, L)),
                ], axis=0)
                for m in range(width)
            ])
            add_rows(8, 0)
            ghost(12)
            add_columns(8)
            for r in range(R):
                rden[r] = 1.0 / (Y[8, r] + 1.0)

        head = lax.broadcasted_iota(jnp.int32, (4, L), 0) == 0

        for k in range(3):
            for m in range(width):
                HQ[k, m : m + 1, :] = low_in[it, m, 1 + k : 2 + k, :]
                HQ[k, 4 + m : 5 + m, :] = high_in[it, m, 1 + k : 2 + k, :]
        half = (HQ[0] - HQ[1]) * 0.5
        tau = jnp.sqrt(half * half + HQ[2] * HQ[2] + 0.25)
        over = jnp.maximum((tau + 0.35 * (HQ[0] + HQ[1])) * HL[1], 1.0)
        HQ[3] = factor * (HL[0] * (1.0 - 1.0 / over))

        def local_rows(ref, side_at, m):
            fq = HQ[3, side_at + m : side_at + m + 1, :]
            return ref[it, m] * (1.0 - fq) + jnp.where(head, fq, 0.0)

        row_correction([
            jnp.concatenate([local_rows(low_in, 0, m), local_rows(high_in, 4, width - 1 - m)], axis=0)
            for m in range(width)
        ])
        for k in range(2):
            for p in range(R + 2 * width):
                g = G[k, p]
                G[k, p] = g + factor * pltpu.roll(g, LANES - 16, 1)
        for f in range(4):
            add_rows(f, f)
            ghost(3 * f)
            add_columns(f)
            for r in range(R):
                state[f, r] = (0.5 * ocean[r]) * (Z[f, r] + Y[f, r] * rden[r])
        return carry

    lax.fori_loop(0, ITERS, iteration, 0)
    outputs = (damage_ref, stress_ref.at[0], stress_ref.at[1], stress_ref.at[2])
    for t in range(tiles):
        cut = slice(t * LANES, t * LANES + span[t])
        for k, target in enumerate(outputs):
            for r in range(R):
                stage[k, t, pl.ds(r, SUB, stride=R), :] = state[k, r, :, t * LANES : (t + 1) * LANES]
            target[:, cut] = stage[k, t, :, : span[t]]


def shards(nlon, nlat, strain_rate, stress_start, concentration, cell_class, land_mask, fold_partner, kernel_weights):
    ncols, nrows = concentration.shape
    side = kernel_weights.shape[0]
    width = side // 2
    R = ncols // SUB
    L = -(-(nrows + 2 * width) // LANES) * LANES
    n = nlon * nlat
    V = lambda *shape: pltpu.VMEM(shape, F32)
    S = lambda *shape: pltpu.SemaphoreType.DMA(shape)
    planes = R + 2 * width
    stress, damage, mean = pl.pallas_call(
        functools.partial(kernel, nlon, nlat, nrows, R, L, side),
        out_shape=(
            jax.ShapeDtypeStruct((3, ncols, nrows), F32),
            jax.ShapeDtypeStruct((ncols, nrows), F32),
            jax.ShapeDtypeStruct((ITERS, LANES), F32),
        ),
        in_specs=[pl.BlockSpec(memory_space=pltpu.SMEM)] * 2 + [pl.BlockSpec(memory_space=pltpu.HBM)] * 5,
        out_specs=(pl.BlockSpec(memory_space=pltpu.VMEM),) * 3,
        scratch_shapes=[
            V(9, R, SUB, L), V(9, R, SUB, L), V(planes, SUB, L),
            V(3, R, SUB, L), V(R, SUB, L), V(R, SUB, L), V(R, SUB, L), V(R, SUB, L), V(4, R, SUB, L),
            V(width, SUB, L), V(2, planes, SUB, LANES), V(planes, SUB, LANES),
            V(-(-(ncols + 2 * width) // SUB) * SUB, LANES),
            V(ITERS, width, 4, L), V(ITERS, width, 4, L), V(ITERS, width, 4, L), V(ITERS, width, 4, L),
            V(2, SUB, L), V(2, SUB, L),
            V(ITERS, 2, SUB, LANES), V(ITERS, 3, SUB, LANES), V(ITERS, nlon, SUB, LANES),
            V(ITERS, 2, LANES), V(ITERS, n, 2, LANES), V(9, L // LANES, ncols, LANES), V(nlon, R, SUB, LANES),
            V(4, SUB, L), V(2, SUB, L), V(3, ncols, nrows), V(3, ncols, nrows), V(ncols, nrows),
            pltpu.VMEM((ncols, nrows), jnp.int32), pltpu.VMEM((ncols, nrows), jnp.int32), S(5),
            S(ITERS, 2), S(ITERS, 2), S(2), S(2), S(ITERS, 3), S(ITERS, 3), S(ITERS, nlon), S(ITERS, nlon),
            S(ITERS, n), S(ITERS, n),
        ],
        compiler_params=pltpu.CompilerParams(
            collective_id=0, has_side_effects=True, vmem_limit_bytes=67043328
        ),
    )(kernel_weights, fold_partner, strain_rate, stress_start, concentration, cell_class, land_mask)
    return stress, damage, mean[:, 0]


def solution(mesh):
    in_specs = (
        P(None, "lon", "lat"),
        P(None, "lon", "lat"),
        P("lon", "lat"),
        P(("member", "lon"), "lat"),
        P("lon", "lat"),
        P(),
        P(),
    )
    out_specs = (P(None, ("member", "lon"), "lat"), P(("member", "lon"), "lat"), P("member"))
    body = functools.partial(shards, mesh.shape["lon"], mesh.shape["lat"])
    return jax.shard_map(body, mesh=mesh, in_specs=in_specs, out_specs=out_specs, check_vma=False)
```

```python
import functools

import jax
import jax.numpy as jnp
from jax import lax
from jax.experimental import pallas as pl
from jax.experimental.pallas import tpu as pltpu
from jax.sharding import PartitionSpec as P

ITERS = 3
LANES = 128
SUB = 8
MESH = pl.DeviceIdType.MESH
F32 = jnp.float32


def kernel(
    nlon, nlat, nrows, R, L, side,
    w_ref, partner_ref, e_hbm, s_hbm, conc_hbm, class_hbm, mask_hbm,
    stress_ref, damage_ref, mean_ref,
    Z, Y, X, load, base, ocean, rlim, rden, state, C, G, XC, D,
    up_out, down_out, low_in, high_in, ocean_out, ocean_in,
    slab, lat_in, fold_in, stat, stat_in, stage, tops, HQ, HL,
    e_ref, s_ref, conc_ref, class_ref, mask_ref, in_sem,
    row_send, row_recv, oc_send, oc_recv, lat_send, lat_recv, fold_send, fold_recv, stat_send, stat_recv,
):
    width = side // 2
    n = nlon * nlat
    ncols = R * SUB
    lon, lat = lax.axis_index("lon"), lax.axis_index("lat")
    member = lax.axis_index("member")
    is_last = lat == nlat - 1
    me = lon * nlat + lat
    nb = nrows - (L - LANES)

    def dev(a, b):
        return (member, a, b)

    def peer(d):
        other = lax.rem(me + d, n)
        return dev(other // nlat, lax.rem(other, nlat))

    right, left = lax.rem(lon + 1, nlon), lax.rem(lon + nlon - 1, nlon)
    other_lat = lax.rem(lat + 1, nlat)

    loads = [
        pltpu.make_async_copy(a, b, in_sem.at[k])
        for k, (a, b) in enumerate((
            (mask_hbm, mask_ref), (conc_hbm, conc_ref), (class_hbm, class_ref), (s_hbm, s_ref), (e_hbm, e_ref)
        ))
    ]
    for copy in loads:
        copy.start()
    barrier = pltpu.get_barrier_semaphore()

    def greet(d, c):
        pl.semaphore_signal(barrier, inc=1, device_id=peer(d), device_id_type=MESH)
        return c

    lax.fori_loop(1, n, greet, 0)

    sub = lax.broadcasted_iota(jnp.int32, (SUB, L), 0)
    lane = lax.broadcasted_iota(jnp.int32, (SUB, LANES), 1)

    for ref in (load, base, ocean, rlim, state, stage):
        ref[...] = jnp.zeros(ref.shape, F32)
    slab[...] = jnp.zeros(slab.shape, F32)
    ocean_out[...] = jnp.zeros(ocean_out.shape, F32)
    HQ[...] = jnp.zeros(HQ.shape, F32)
    HL[...] = jnp.zeros(HL.shape, F32)
    for copy in loads:
        copy.wait()
    tiles = L // LANES
    span = [min(LANES, nrows - t * LANES) for t in range(tiles)]
    sources = (
        mask_ref, conc_ref, class_ref, s_ref.at[0], s_ref.at[1], s_ref.at[2], e_ref.at[0], e_ref.at[1], e_ref.at[2]
    )
    for t in range(tiles):
        cut = slice(t * LANES, t * LANES + span[t])
        for k, source in enumerate(sources):
            stage[k, t, :, : span[t]] = source[:, cut].astype(F32)
        for r in range(R):
            oc, conc, grade, s1, s2, s3, one, two, shear = (
                stage[k, t, pl.ds(r, SUB, stride=R), :][:, : span[t]] for k in range(9)
            )
            ocean[r, :, cut] = oc
            base[r, :, cut] = conc * jnp.exp(-2.0 * (1.0 - conc))
            rlim[r, :, cut] = 1.0 / (0.6 * conc)
            state[0, r, :, cut] = oc * 0.1 * grade * conc
            for k, part in enumerate((s1, s2, s3)):
                state[1 + k, r, :, cut] = oc * part
            load[0, r, :, cut] = (one + two / 3.0) / (8.0 / 9.0)
            load[1, r, :, cut] = (two + one / 3.0) / (8.0 / 9.0)
            load[2, r, :, cut] = (shear / (4.0 / 3.0)) / (8.0 / 9.0)
    count = jnp.zeros((1, L), F32)
    for r in range(R):
        Z[8, r] = ocean[r]
        count = count + jnp.sum(ocean[r], axis=0, keepdims=True)
    count = functools.reduce(
        lambda a, b: a + b, [count[:, t * LANES : (t + 1) * LANES] for t in range(L // LANES)]
    )
    for m in range(width):
        ocean_out[0, 4 + m : 5 + m, :] = rlim[R - width + m, SUB - 1 : SUB, :]
        ocean_out[1, 4 + m : 5 + m, :] = rlim[m, 0:1, :]
        ocean_out[0, m : m + 1, :] = ocean[R - width + m, SUB - 1 : SUB, :]
        ocean_out[1, m : m + 1, :] = ocean[m, 0:1, :]

    pl.semaphore_wait(barrier, n - 1)

    def ocean_copy(k, to):
        return pltpu.make_async_remote_copy(
            src_ref=ocean_out.at[k], dst_ref=ocean_in.at[k], send_sem=oc_send.at[k],
            recv_sem=oc_recv.at[k], device_id=dev(to, lat), device_id_type=MESH,
        )

    ocean_copy(0, right).start()
    ocean_copy(1, left).start()

    def conv(f, c):
        for r in range(R):
            X[width + r] = Z[f, r]
        for m in range(width):
            X[m] = jnp.where(sub == 0, 0.0, pltpu.roll(Z[f, m + R - width], 1, 0))
            X[R + width + m] = jnp.where(sub == SUB - 1, 0.0, pltpu.roll(Z[f, m], SUB - 1, 0))
        for b in range(side):
            acc = [None] * R
            for p in range(R + 2 * width):
                x = X[p]
                for r in range(R):
                    a = p - r
                    if 0 <= a < side:
                        term = w_ref[a, b] * x
                        acc[r] = term if acc[r] is None else acc[r] + term
            for r in range(R):
                moved = acc[r] if b == width else pltpu.roll(acc[r], (width - b) % L, 1)
                if b == 0:
                    Y[f, r] = moved
                else:
                    Y[f, r] = Y[f, r] + moved
        return c

    def row_correction(halos):
        for r in range(width):
            total = None
            for b in range(side):
                t = None
                for m in range(r, width):
                    d = m - r
                    w = jnp.where(sub < 4, w_ref[d, b], w_ref[side - 1 - d, b])
                    term = w * halos[m]
                    t = term if t is None else t + term
                t = t if b == width else pltpu.roll(t, (width - b) % L, 1)
                total = t if total is None else total + t
            C[r] = total

    def add_rows(f, c):
        for r in range(width):
            Y[f, r] = Y[f, r] + jnp.where(sub == 0, C[r, c : c + 1, :], 0.0)
            Y[f, R - 1 - r] = Y[f, R - 1 - r] + jnp.where(sub == SUB - 1, C[r, 4 + c : 5 + c, :], 0.0)

    def add_columns(f):
        for r in range(R):
            total = None
            for b in range(side):
                t = None
                for a in range(side):
                    term = w_ref[a, b] * XC[r + a]
                    t = term if t is None else t + term
                t = t if b == width else pltpu.roll(t, (width - b) % LANES, 1)
                total = t if total is None else total + t
            Y[f, r, :, L - LANES :] = Y[f, r, :, L - LANES :] + jnp.where(
                (lane >= nb - width) & (lane < nb), total, 0.0
            )
            Y[f, r, :, :LANES] = Y[f, r, :, :LANES] + jnp.where(lane < width, total, 0.0)

    def ghost(at):
        for p in range(R + 2 * width):
            north = pltpu.roll(G[1, p], (nb - at) % LANES, 1)
            south = jnp.where(lat > 0, pltpu.roll(G[0, p], (LANES - width - at) % LANES, 1), 0.0)
            XC[p] = jnp.where(
                (lane >= nb) & (lane < nb + width), north,
                jnp.where(lane >= LANES - width, south, 0.0),
            )

    def iteration(it, carry):
        excess = jnp.zeros((SUB, L), F32)
        for r in range(R):
            oc = ocean[r]
            damage = state[0, r]
            keep = 1.0 - damage
            theta = 0.5 / (keep * keep)
            scale = oc / (1.0 + theta)
            bk = base[r] * keep
            el = [scale * (state[1 + k, r] + bk * load[k, r]) for k in range(3)]
            half = (el[0] - el[1]) * 0.5
            tau = jnp.sqrt(half * half + el[2] * el[2] + 0.25)
            over = jnp.maximum((tau + 0.35 * (el[0] + el[1])) * rlim[r], 1.0)
            q = oc * (1.0 - 1.0 / over)
            excess = excess + oc * (over - 1.0)
            Z[0, r] = damage
            Z[4, r] = keep * q
            for k in range(3):
                Z[1 + k, r] = el[k]
                Z[5 + k, r] = -(el[k] * q)
        for m in range(width):
            hi = R - width + m
            for f in range(4):
                up_out[it, m, f : f + 1, :] = Z[f, hi, SUB - 1 : SUB, :]
                down_out[it, m, f : f + 1, :] = Z[f, m, 0:1, :]
        up = pltpu.make_async_remote_copy(
            src_ref=up_out.at[it], dst_ref=low_in.at[it], send_sem=row_send.at[it, 0],
            recv_sem=row_recv.at[it, 0], device_id=dev(right, lat), device_id_type=MESH,
        )
        down = pltpu.make_async_remote_copy(
            src_ref=down_out.at[it], dst_ref=high_in.at[it], send_sem=row_send.at[it, 1],
            recv_sem=row_recv.at[it, 1], device_id=dev(left, lat), device_id_type=MESH,
        )
        lines = jnp.sum(excess, axis=0, keepdims=True)
        stat[it, 0:1, :] = functools.reduce(
            lambda a, b: a + b, [lines[:, t * LANES : (t + 1) * LANES] for t in range(L // LANES)]
        )
        stat[it, 1:2, :] = count

        def stat_copy(d):
            return pltpu.make_async_remote_copy(
                src_ref=stat.at[it], dst_ref=stat_in.at[it, d], send_sem=stat_send.at[it, d],
                recv_sem=stat_recv.at[it, d], device_id=peer(d), device_id_type=MESH,
            )

        def start_stat(d, c):
            stat_copy(d).start()
            return c

        lax.fori_loop(1, n, start_stat, 0)
        up.start()
        down.start()

        edge = jnp.zeros((SUB, LANES), F32)
        top = jnp.zeros((SUB, LANES), F32)
        for r in range(R):
            for f in range(9):
                at = 32 * r + (3 * f if f < 4 else (16 + 3 * (f - 4) if f < 8 else 12))
                first = Z[f, r, :, :LANES]
                last = Z[f, r, :, L - LANES :]
                both = jnp.where(
                    is_last, pltpu.roll(first, at, 1), pltpu.roll(last, (at + width - nb) % LANES, 1)
                )
                edge = jnp.where((lane >= at) & (lane < at + width), both, edge)
                for k in range(width):
                    top = jnp.where(lane == at + k, pltpu.roll(last, (at + k - (nb - 1 - k)) % LANES, 1), top)
        slab[it, 0] = edge
        slab[it, 1] = top

        def lat_copy(k):
            to = lax.rem(lon + 1 - k + nlon, nlon)
            return pltpu.make_async_remote_copy(
                src_ref=slab.at[it, 0], dst_ref=lat_in.at[it, k], send_sem=lat_send.at[it, k],
                recv_sem=lat_recv.at[it, k], device_id=dev(to, other_lat), device_id_type=MESH,
            )

        def fold_copy(d):
            return pltpu.make_async_remote_copy(
                src_ref=slab.at[it, 1], dst_ref=fold_in.at[it, lon],
                send_sem=fold_send.at[it, d], recv_sem=fold_recv.at[it, d],
                device_id=dev(lax.rem(lon + d, nlon), lat), device_id_type=MESH,
            )

        for k in range(3):
            lat_copy(k).start()

        @pl.when(is_last)
        def _():
            def start_fold(d, c):
                fold_copy(d).start()
                return c

            lax.fori_loop(1, nlon, start_fold, 0)
            fold_in[it, lon] = slab[it, 1]

        lax.fori_loop(0, jnp.where(it == 0, 9, 8), conv, 0)

        def wait_stat(d, c):
            stat_copy(d).wait()
            return c

        lax.fori_loop(1, n, wait_stat, 0)
        stat_in[it, 0] = stat[it]

        def add_stat(d, total):
            return total + stat_in[it, d]

        total = lax.fori_loop(1, n, add_stat, stat_in[it, 0])
        sums = jnp.sum(total, axis=1, keepdims=True)
        mean = sums[0:1] / (sums[1:2] + 1.0)
        factor = 1.0 / (1.0 + 2.0 * mean)
        mean_ref[it] = mean[0, 0]

        for f in range(4):
            for r in range(R):
                Y[f, r] = Y[f, r] + factor * Y[4 + f, r]
                Z[f, r] = Z[f, r] + factor * Z[4 + f, r]

        up.wait()
        down.wait()
        for k in range(3):
            lat_copy(k).wait()

        @pl.when(is_last)
        def _():
            def wait_fold(d, c):
                fold_copy(d).wait()
                return c

            lax.fori_loop(1, nlon, wait_fold, 0)

            def spread(k, c):
                tile = fold_in[it, k]
                for r in range(R):
                    tops[k, r] = tile if r == 0 else pltpu.roll(tile, LANES - 32 * r, 1)
                return c

            lax.fori_loop(0, nlon, spread, 0)

            def pick(i, c):
                where = lax.rem(lon * ncols + i - width + nlon * ncols, nlon * ncols)
                p = partner_ref[where]
                col = lax.rem(p, ncols)
                D[pl.ds(i, 1), :] = tops[p // ncols, lax.rem(col, R), pl.ds(col // R, 1), :]
                return c

            lax.fori_loop(0, ncols + 2 * width, pick, 0, unroll=True)
            for p in range(R + 2 * width):
                G[1, p] = D[pl.ds(p, SUB, stride=R), :]

        @pl.when(jnp.logical_not(is_last))
        def _():
            for p in range(R + 2 * width):
                G[1, p] = jnp.zeros((SUB, LANES), F32)

        small = lax.broadcasted_iota(jnp.int32, (SUB, LANES), 0)
        def piece(k, r):
            return lat_in[it, k] if r == 0 else pltpu.roll(lat_in[it, k], LANES - 32 * r, 1)

        own = [piece(1, r) for r in range(R)]
        for r in range(R):
            G[0, width + r] = own[r]
        for m in range(width):
            r = m + R - width
            G[0, m] = jnp.where(small == 0, pltpu.roll(piece(0, r), 1, 0), pltpu.roll(own[r], 1, 0))
            G[0, R + width + m] = jnp.where(
                small == SUB - 1, pltpu.roll(piece(2, m), SUB - 1, 0), pltpu.roll(own[m], SUB - 1, 0)
            )
        for p in range(R + 2 * width):
            G[1, p] = jnp.where(is_last, G[1, p], G[0, p])

        @pl.when(it == 0)
        def _():
            ocean_copy(0, right).wait()
            ocean_copy(1, left).wait()
            for k in range(2):
                for m in range(width):
                    HL[k, m : m + 1, :] = ocean_in[0, 4 * k + m : 4 * k + m + 1, :]
                    HL[k, 4 + m : 5 + m, :] = ocean_in[1, 4 * k + m : 4 * k + m + 1, :]
            row_correction([
                jnp.concatenate([
                    jnp.broadcast_to(ocean_in[0, m : m + 1, :], (4, L)),
                    jnp.broadcast_to(ocean_in[1, width - 1 - m : width - m, :], (4, L)),
                ], axis=0)
                for m in range(width)
            ])
            add_rows(8, 0)
            ghost(12)
            add_columns(8)
            for r in range(R):
                rden[r] = 1.0 / (Y[8, r] + 1.0)

        head = lax.broadcasted_iota(jnp.int32, (4, L), 0) == 0

        for k in range(3):
            for m in range(width):
                HQ[k, m : m + 1, :] = low_in[it, m, 1 + k : 2 + k, :]
                HQ[k, 4 + m : 5 + m, :] = high_in[it, m, 1 + k : 2 + k, :]
        half = (HQ[0] - HQ[1]) * 0.5
        tau = jnp.sqrt(half * half + HQ[2] * HQ[2] + 0.25)
        over = jnp.maximum((tau + 0.35 * (HQ[0] + HQ[1])) * HL[1], 1.0)
        HQ[3] = factor * (HL[0] * (1.0 - 1.0 / over))

        def local_rows(ref, side_at, m):
            fq = HQ[3, side_at + m : side_at + m + 1, :]
            return ref[it, m] * (1.0 - fq) + jnp.where(head, fq, 0.0)

        row_correction([
            jnp.concatenate([local_rows(low_in, 0, m), local_rows(high_in, 4, width - 1 - m)], axis=0)
            for m in range(width)
        ])
        for k in range(2):
            for p in range(R + 2 * width):
                g = G[k, p]
                G[k, p] = g + factor * pltpu.roll(g, LANES - 16, 1)
        for f in range(4):
            add_rows(f, f)
            ghost(3 * f)
            add_columns(f)
            for r in range(R):
                state[f, r] = (0.5 * ocean[r]) * (Z[f, r] + Y[f, r] * rden[r])
        return carry

    lax.fori_loop(0, ITERS, iteration, 0)
    outputs = (damage_ref, stress_ref.at[0], stress_ref.at[1], stress_ref.at[2])
    for t in range(tiles):
        cut = slice(t * LANES, t * LANES + span[t])
        for k, target in enumerate(outputs):
            for r in range(R):
                stage[k, t, pl.ds(r, SUB, stride=R), :] = state[k, r, :, t * LANES : (t + 1) * LANES]
            target[:, cut] = stage[k, t, :, : span[t]]


def shards(nlon, nlat, strain_rate, stress_start, concentration, cell_class, land_mask, fold_partner, kernel_weights):
    ncols, nrows = concentration.shape
    side = kernel_weights.shape[0]
    width = side // 2
    R = ncols // SUB
    L = -(-(nrows + 2 * width) // LANES) * LANES
    n = nlon * nlat
    V = lambda *shape: pltpu.VMEM(shape, F32)
    S = lambda *shape: pltpu.SemaphoreType.DMA(shape)
    planes = R + 2 * width
    stress, damage, mean = pl.pallas_call(
        functools.partial(kernel, nlon, nlat, nrows, R, L, side),
        out_shape=(
            pltpu.VMEM((3, ncols, nrows), F32),
            pltpu.VMEM((ncols, nrows), F32),
            jax.ShapeDtypeStruct((ITERS,), F32),
        ),
        in_specs=[pl.BlockSpec(memory_space=pltpu.SMEM)] * 2 + [pl.BlockSpec(memory_space=pltpu.HBM)] * 5,
        out_specs=(pl.BlockSpec(memory_space=pltpu.VMEM),) * 2 + (pl.BlockSpec(memory_space=pltpu.SMEM),),
        scratch_shapes=[
            V(9, R, SUB, L), V(9, R, SUB, L), V(planes, SUB, L),
            V(3, R, SUB, L), V(R, SUB, L), V(R, SUB, L), V(R, SUB, L), V(R, SUB, L), V(4, R, SUB, L),
            V(width, SUB, L), V(2, planes, SUB, LANES), V(planes, SUB, LANES),
            V(-(-(ncols + 2 * width) // SUB) * SUB, LANES),
            V(ITERS, width, 4, L), V(ITERS, width, 4, L), V(ITERS, width, 4, L), V(ITERS, width, 4, L),
            V(2, SUB, L), V(2, SUB, L),
            V(ITERS, 2, SUB, LANES), V(ITERS, 3, SUB, LANES), V(ITERS, nlon, SUB, LANES),
            V(ITERS, 2, LANES), V(ITERS, n, 2, LANES), V(9, L // LANES, ncols, LANES), V(nlon, R, SUB, LANES),
            V(4, SUB, L), V(2, SUB, L), V(3, ncols, nrows), V(3, ncols, nrows), V(ncols, nrows),
            pltpu.VMEM((ncols, nrows), jnp.int32), pltpu.VMEM((ncols, nrows), jnp.int32), S(5),
            S(ITERS, 2), S(ITERS, 2), S(2), S(2), S(ITERS, 3), S(ITERS, 3), S(ITERS, nlon), S(ITERS, nlon),
            S(ITERS, n), S(ITERS, n),
        ],
        compiler_params=pltpu.CompilerParams(
            collective_id=0, has_side_effects=True, vmem_limit_bytes=67043328 - 1024 * 1024
        ),
    )(kernel_weights, fold_partner, strain_rate, stress_start, concentration, cell_class, land_mask)
    return stress, damage, mean


def solution(mesh):
    in_specs = (
        P(None, "lon", "lat"),
        P(None, "lon", "lat"),
        P("lon", "lat"),
        P(("member", "lon"), "lat"),
        P("lon", "lat"),
        P(),
        P(),
    )
    out_specs = (P(None, ("member", "lon"), "lat"), P(("member", "lon"), "lat"), P("member"))
    body = functools.partial(shards, mesh.shape["lon"], mesh.shape["lat"])
    return jax.shard_map(body, mesh=mesh, in_specs=in_specs, out_specs=out_specs, check_vma=False)
```

```python
import functools

import jax
import jax.numpy as jnp
from jax import lax
from jax.experimental import pallas as pl
from jax.experimental.pallas import tpu as pltpu
from jax.sharding import PartitionSpec as P

ITERS = 3
LANES = 128
SUB = 8
MESH = pl.DeviceIdType.MESH
F32 = jnp.float32


def kernel(
    nlon, nlat, nrows, R, L, side,
    w_ref, partner_ref, e_hbm, s_hbm, conc_hbm, class_hbm, mask_hbm,
    stress_ref, damage_ref, mean_ref,
    Z, Y, X, load, base, ocean, rlim, rden, state, C, G, XC, D,
    up_out, down_out, low_in, high_in, ocean_out, ocean_in,
    slab, lat_in, fold_in, stat, stat_in, stage, tops, HQ, HL,
    e_ref, s_ref, conc_ref, class_ref, mask_ref, in_sem,
    row_send, row_recv, oc_send, oc_recv, lat_send, lat_recv, fold_send, fold_recv, stat_send, stat_recv,
):
    width = side // 2
    n = nlon * nlat
    ncols = R * SUB
    lon, lat = lax.axis_index("lon"), lax.axis_index("lat")
    member = lax.axis_index("member")
    is_last = lat == nlat - 1
    me = lon * nlat + lat
    nb = nrows - (L - LANES)

    def dev(a, b):
        return (member, a, b)

    def peer(d):
        other = lax.rem(me + d, n)
        return dev(other // nlat, lax.rem(other, nlat))

    right, left = lax.rem(lon + 1, nlon), lax.rem(lon + nlon - 1, nlon)
    other_lat = lax.rem(lat + 1, nlat)

    loads = [
        pltpu.make_async_copy(a, b, in_sem.at[k])
        for k, (a, b) in enumerate((
            (mask_hbm, mask_ref), (conc_hbm, conc_ref), (class_hbm, class_ref), (s_hbm, s_ref), (e_hbm, e_ref)
        ))
    ]
    for copy in loads:
        copy.start()
    barrier = pltpu.get_barrier_semaphore()

    def greet(d, c):
        pl.semaphore_signal(barrier, inc=1, device_id=peer(d), device_id_type=MESH)
        return c

    lax.fori_loop(1, n, greet, 0)

    sub = lax.broadcasted_iota(jnp.int32, (SUB, L), 0)
    lane = lax.broadcasted_iota(jnp.int32, (SUB, LANES), 1)

    for ref in (load, base, ocean, rlim, state, stage):
        ref[...] = jnp.zeros(ref.shape, F32)
    slab[...] = jnp.zeros(slab.shape, F32)
    ocean_out[...] = jnp.zeros(ocean_out.shape, F32)
    HQ[...] = jnp.zeros(HQ.shape, F32)
    HL[...] = jnp.zeros(HL.shape, F32)
    for copy in loads:
        copy.wait()
    tiles = L // LANES
    span = [min(LANES, nrows - t * LANES) for t in range(tiles)]
    sources = (
        mask_ref, conc_ref, class_ref, s_ref.at[0], s_ref.at[1], s_ref.at[2], e_ref.at[0], e_ref.at[1], e_ref.at[2]
    )
    for t in range(tiles):
        cut = slice(t * LANES, t * LANES + span[t])
        for k, source in enumerate(sources):
            stage[k, t, :, : span[t]] = source[:, cut].astype(F32)
        for r in range(R):
            oc, conc, grade, s1, s2, s3, one, two, shear = (
                stage[k, t, pl.ds(r, SUB, stride=R), :][:, : span[t]] for k in range(9)
            )
            ocean[r, :, cut] = oc
            base[r, :, cut] = conc * jnp.exp(-2.0 * (1.0 - conc))
            rlim[r, :, cut] = 1.0 / (0.6 * conc)
            state[0, r, :, cut] = oc * 0.1 * grade * conc
            for k, part in enumerate((s1, s2, s3)):
                state[1 + k, r, :, cut] = oc * part
            load[0, r, :, cut] = (one + two / 3.0) / (8.0 / 9.0)
            load[1, r, :, cut] = (two + one / 3.0) / (8.0 / 9.0)
            load[2, r, :, cut] = (shear / (4.0 / 3.0)) / (8.0 / 9.0)
    count = jnp.zeros((1, L), F32)
    for r in range(R):
        Z[8, r] = ocean[r]
        count = count + jnp.sum(ocean[r], axis=0, keepdims=True)
    count = functools.reduce(
        lambda a, b: a + b, [count[:, t * LANES : (t + 1) * LANES] for t in range(L // LANES)]
    )
    for m in range(width):
        ocean_out[0, 4 + m : 5 + m, :] = rlim[R - width + m, SUB - 1 : SUB, :]
        ocean_out[1, 4 + m : 5 + m, :] = rlim[m, 0:1, :]
        ocean_out[0, m : m + 1, :] = ocean[R - width + m, SUB - 1 : SUB, :]
        ocean_out[1, m : m + 1, :] = ocean[m, 0:1, :]

    pl.semaphore_wait(barrier, n - 1)

    def ocean_copy(k, to):
        return pltpu.make_async_remote_copy(
            src_ref=ocean_out.at[k], dst_ref=ocean_in.at[k], send_sem=oc_send.at[k],
            recv_sem=oc_recv.at[k], device_id=dev(to, lat), device_id_type=MESH,
        )

    ocean_copy(0, right).start()
    ocean_copy(1, left).start()

    def conv(f, c):
        for r in range(R):
            X[width + r] = Z[f, r]
        for m in range(width):
            X[m] = jnp.where(sub == 0, 0.0, pltpu.roll(Z[f, m + R - width], 1, 0))
            X[R + width + m] = jnp.where(sub == SUB - 1, 0.0, pltpu.roll(Z[f, m], SUB - 1, 0))
        for b in range(side):
            acc = [None] * R
            for p in range(R + 2 * width):
                x = X[p]
                for r in range(R):
                    a = p - r
                    if 0 <= a < side:
                        term = w_ref[a, b] * x
                        acc[r] = term if acc[r] is None else acc[r] + term
            for r in range(R):
                moved = acc[r] if b == width else pltpu.roll(acc[r], (width - b) % L, 1)
                if b == 0:
                    Y[f, r] = moved
                else:
                    Y[f, r] = Y[f, r] + moved
        return c

    def row_correction(halos):
        for r in range(width):
            total = None
            for b in range(side):
                t = None
                for m in range(r, width):
                    d = m - r
                    w = jnp.where(sub < 4, w_ref[d, b], w_ref[side - 1 - d, b])
                    term = w * halos[m]
                    t = term if t is None else t + term
                t = t if b == width else pltpu.roll(t, (width - b) % L, 1)
                total = t if total is None else total + t
            C[r] = total

    def add_rows(f, c):
        for r in range(width):
            Y[f, r] = Y[f, r] + jnp.where(sub == 0, C[r, c : c + 1, :], 0.0)
            Y[f, R - 1 - r] = Y[f, R - 1 - r] + jnp.where(sub == SUB - 1, C[r, 4 + c : 5 + c, :], 0.0)

    def add_columns(f):
        for r in range(R):
            total = None
            for b in range(side):
                t = None
                for a in range(side):
                    term = w_ref[a, b] * XC[r + a]
                    t = term if t is None else t + term
                t = t if b == width else pltpu.roll(t, (width - b) % LANES, 1)
                total = t if total is None else total + t
            Y[f, r, :, L - LANES :] = Y[f, r, :, L - LANES :] + jnp.where(
                (lane >= nb - width) & (lane < nb), total, 0.0
            )
            Y[f, r, :, :LANES] = Y[f, r, :, :LANES] + jnp.where(lane < width, total, 0.0)

    def ghost(at):
        for p in range(R + 2 * width):
            north = pltpu.roll(G[1, p], (nb - at) % LANES, 1)
            south = jnp.where(lat > 0, pltpu.roll(G[0, p], (LANES - width - at) % LANES, 1), 0.0)
            XC[p] = jnp.where(
                (lane >= nb) & (lane < nb + width), north,
                jnp.where(lane >= LANES - width, south, 0.0),
            )

    def iteration(it, carry):
        excess = jnp.zeros((SUB, L), F32)
        for r in range(R):
            oc = ocean[r]
            damage = state[0, r]
            keep = 1.0 - damage
            theta = 0.5 / (keep * keep)
            scale = oc / (1.0 + theta)
            bk = base[r] * keep
            el = [scale * (state[1 + k, r] + bk * load[k, r]) for k in range(3)]
            half = (el[0] - el[1]) * 0.5
            tau = jnp.sqrt(half * half + el[2] * el[2] + 0.25)
            over = jnp.maximum((tau + 0.35 * (el[0] + el[1])) * rlim[r], 1.0)
            q = oc * (1.0 - 1.0 / over)
            excess = excess + oc * (over - 1.0)
            Z[0, r] = damage
            Z[4, r] = keep * q
            for k in range(3):
                Z[1 + k, r] = el[k]
                Z[5 + k, r] = -(el[k] * q)
        for m in range(width):
            hi = R - width + m
            for f in range(4):
                up_out[it, m, f : f + 1, :] = Z[f, hi, SUB - 1 : SUB, :]
                down_out[it, m, f : f + 1, :] = Z[f, m, 0:1, :]
        up = pltpu.make_async_remote_copy(
            src_ref=up_out.at[it], dst_ref=low_in.at[it], send_sem=row_send.at[it, 0],
            recv_sem=row_recv.at[it, 0], device_id=dev(right, lat), device_id_type=MESH,
        )
        down = pltpu.make_async_remote_copy(
            src_ref=down_out.at[it], dst_ref=high_in.at[it], send_sem=row_send.at[it, 1],
            recv_sem=row_recv.at[it, 1], device_id=dev(left, lat), device_id_type=MESH,
        )
        lines = jnp.sum(excess, axis=0, keepdims=True)
        stat[it, 0:1, :] = functools.reduce(
            lambda a, b: a + b, [lines[:, t * LANES : (t + 1) * LANES] for t in range(L // LANES)]
        )
        stat[it, 1:2, :] = count

        def stat_copy(d):
            return pltpu.make_async_remote_copy(
                src_ref=stat.at[it], dst_ref=stat_in.at[it, d], send_sem=stat_send.at[it, d],
                recv_sem=stat_recv.at[it, d], device_id=peer(d), device_id_type=MESH,
            )

        def start_stat(d, c):
            stat_copy(d).start()
            return c

        lax.fori_loop(1, n, start_stat, 0)
        up.start()
        down.start()

        edge = jnp.zeros((SUB, LANES), F32)
        top = jnp.zeros((SUB, LANES), F32)
        for r in range(R):
            for f in range(9):
                at = 32 * r + (3 * f if f < 4 else (16 + 3 * (f - 4) if f < 8 else 12))
                first = Z[f, r, :, :LANES]
                last = Z[f, r, :, L - LANES :]
                both = jnp.where(
                    is_last, pltpu.roll(first, at, 1), pltpu.roll(last, (at + width - nb) % LANES, 1)
                )
                edge = jnp.where((lane >= at) & (lane < at + width), both, edge)
                for k in range(width):
                    top = jnp.where(lane == at + k, pltpu.roll(last, (at + k - (nb - 1 - k)) % LANES, 1), top)
        slab[it, 0] = edge
        slab[it, 1] = top

        def lat_copy(k):
            to = lax.rem(lon + 1 - k + nlon, nlon)
            return pltpu.make_async_remote_copy(
                src_ref=slab.at[it, 0], dst_ref=lat_in.at[it, k], send_sem=lat_send.at[it, k],
                recv_sem=lat_recv.at[it, k], device_id=dev(to, other_lat), device_id_type=MESH,
            )

        def fold_copy(d):
            return pltpu.make_async_remote_copy(
                src_ref=slab.at[it, 1], dst_ref=fold_in.at[it, lon],
                send_sem=fold_send.at[it, d], recv_sem=fold_recv.at[it, d],
                device_id=dev(lax.rem(lon + d, nlon), lat), device_id_type=MESH,
            )

        for k in range(3):
            lat_copy(k).start()

        @pl.when(is_last)
        def _():
            def start_fold(d, c):
                fold_copy(d).start()
                return c

            lax.fori_loop(1, nlon, start_fold, 0)
            fold_in[it, lon] = slab[it, 1]

        def early(j, c):
            return conv(j + (j >= 3).astype(jnp.int32) + (j >= 6).astype(jnp.int32), c)

        lax.fori_loop(0, jnp.where(it == 0, 7, 6), early, 0)

        def wait_stat(d, c):
            stat_copy(d).wait()
            return c

        lax.fori_loop(1, n, wait_stat, 0)
        stat_in[it, 0] = stat[it]

        def add_stat(d, total):
            return total + stat_in[it, d]

        total = lax.fori_loop(1, n, add_stat, stat_in[it, 0])
        sums = jnp.sum(total, axis=1, keepdims=True)
        mean = sums[0:1] / (sums[1:2] + 1.0)
        factor = 1.0 / (1.0 + 2.0 * mean)
        mean_ref[it] = mean[0, 0]

        for f in range(4):
            for r in range(R):
                if f < 3:
                    Y[f, r] = Y[f, r] + factor * Y[4 + f, r]
                Z[f, r] = Z[f, r] + factor * Z[4 + f, r]

        lax.fori_loop(3, 4, conv, 0)

        up.wait()
        down.wait()
        for k in range(3):
            lat_copy(k).wait()

        @pl.when(is_last)
        def _():
            def wait_fold(d, c):
                fold_copy(d).wait()
                return c

            lax.fori_loop(1, nlon, wait_fold, 0)

            def spread(k, c):
                tile = fold_in[it, k]
                for r in range(R):
                    tops[k, r] = tile if r == 0 else pltpu.roll(tile, LANES - 32 * r, 1)
                return c

            lax.fori_loop(0, nlon, spread, 0)

            def pick(i, c):
                where = lax.rem(lon * ncols + i - width + nlon * ncols, nlon * ncols)
                p = partner_ref[where]
                col = lax.rem(p, ncols)
                D[pl.ds(i, 1), :] = tops[p // ncols, lax.rem(col, R), pl.ds(col // R, 1), :]
                return c

            lax.fori_loop(0, ncols + 2 * width, pick, 0, unroll=True)
            for p in range(R + 2 * width):
                G[1, p] = D[pl.ds(p, SUB, stride=R), :]

        @pl.when(jnp.logical_not(is_last))
        def _():
            for p in range(R + 2 * width):
                G[1, p] = jnp.zeros((SUB, LANES), F32)

        small = lax.broadcasted_iota(jnp.int32, (SUB, LANES), 0)
        def piece(k, r):
            return lat_in[it, k] if r == 0 else pltpu.roll(lat_in[it, k], LANES - 32 * r, 1)

        own = [piece(1, r) for r in range(R)]
        for r in range(R):
            G[0, width + r] = own[r]
        for m in range(width):
            r = m + R - width
            G[0, m] = jnp.where(small == 0, pltpu.roll(piece(0, r), 1, 0), pltpu.roll(own[r], 1, 0))
            G[0, R + width + m] = jnp.where(
                small == SUB - 1, pltpu.roll(piece(2, m), SUB - 1, 0), pltpu.roll(own[m], SUB - 1, 0)
            )
        for p in range(R + 2 * width):
            G[1, p] = jnp.where(is_last, G[1, p], G[0, p])

        @pl.when(it == 0)
        def _():
            ocean_copy(0, right).wait()
            ocean_copy(1, left).wait()
            for k in range(2):
                for m in range(width):
                    HL[k, m : m + 1, :] = ocean_in[0, 4 * k + m : 4 * k + m + 1, :]
                    HL[k, 4 + m : 5 + m, :] = ocean_in[1, 4 * k + m : 4 * k + m + 1, :]
            row_correction([
                jnp.concatenate([
                    jnp.broadcast_to(ocean_in[0, m : m + 1, :], (4, L)),
                    jnp.broadcast_to(ocean_in[1, width - 1 - m : width - m, :], (4, L)),
                ], axis=0)
                for m in range(width)
            ])
            add_rows(8, 0)
            ghost(12)
            add_columns(8)
            for r in range(R):
                rden[r] = 1.0 / (Y[8, r] + 1.0)

        head = lax.broadcasted_iota(jnp.int32, (4, L), 0) == 0

        for k in range(3):
            for m in range(width):
                HQ[k, m : m + 1, :] = low_in[it, m, 1 + k : 2 + k, :]
                HQ[k, 4 + m : 5 + m, :] = high_in[it, m, 1 + k : 2 + k, :]
        half = (HQ[0] - HQ[1]) * 0.5
        tau = jnp.sqrt(half * half + HQ[2] * HQ[2] + 0.25)
        over = jnp.maximum((tau + 0.35 * (HQ[0] + HQ[1])) * HL[1], 1.0)
        HQ[3] = factor * (HL[0] * (1.0 - 1.0 / over))

        def local_rows(ref, side_at, m):
            fq = HQ[3, side_at + m : side_at + m + 1, :]
            return ref[it, m] * (1.0 - fq) + jnp.where(head, fq, 0.0)

        row_correction([
            jnp.concatenate([local_rows(low_in, 0, m), local_rows(high_in, 4, width - 1 - m)], axis=0)
            for m in range(width)
        ])
        for k in range(2):
            for p in range(R + 2 * width):
                g = G[k, p]
                G[k, p] = g + factor * pltpu.roll(g, LANES - 16, 1)
        for f in range(4):
            add_rows(f, f)
            ghost(3 * f)
            add_columns(f)
            for r in range(R):
                state[f, r] = (0.5 * ocean[r]) * (Z[f, r] + Y[f, r] * rden[r])
        return carry

    lax.fori_loop(0, ITERS, iteration, 0)
    outputs = (damage_ref, stress_ref.at[0], stress_ref.at[1], stress_ref.at[2])
    for t in range(tiles):
        cut = slice(t * LANES, t * LANES + span[t])
        for k, target in enumerate(outputs):
            for r in range(R):
                stage[k, t, pl.ds(r, SUB, stride=R), :] = state[k, r, :, t * LANES : (t + 1) * LANES]
            target[:, cut] = stage[k, t, :, : span[t]]


def shards(nlon, nlat, strain_rate, stress_start, concentration, cell_class, land_mask, fold_partner, kernel_weights):
    ncols, nrows = concentration.shape
    side = kernel_weights.shape[0]
    width = side // 2
    R = ncols // SUB
    L = -(-(nrows + 2 * width) // LANES) * LANES
    n = nlon * nlat
    V = lambda *shape: pltpu.VMEM(shape, F32)
    S = lambda *shape: pltpu.SemaphoreType.DMA(shape)
    planes = R + 2 * width
    stress, damage, mean = pl.pallas_call(
        functools.partial(kernel, nlon, nlat, nrows, R, L, side),
        out_shape=(
            pltpu.VMEM((3, ncols, nrows), F32),
            pltpu.VMEM((ncols, nrows), F32),
            jax.ShapeDtypeStruct((ITERS,), F32),
        ),
        in_specs=[pl.BlockSpec(memory_space=pltpu.SMEM)] * 2 + [pl.BlockSpec(memory_space=pltpu.HBM)] * 5,
        out_specs=(pl.BlockSpec(memory_space=pltpu.VMEM),) * 2 + (pl.BlockSpec(memory_space=pltpu.SMEM),),
        scratch_shapes=[
            V(9, R, SUB, L), V(9, R, SUB, L), V(planes, SUB, L),
            V(3, R, SUB, L), V(R, SUB, L), V(R, SUB, L), V(R, SUB, L), V(R, SUB, L), V(4, R, SUB, L),
            V(width, SUB, L), V(2, planes, SUB, LANES), V(planes, SUB, LANES),
            V(-(-(ncols + 2 * width) // SUB) * SUB, LANES),
            V(ITERS, width, 4, L), V(ITERS, width, 4, L), V(ITERS, width, 4, L), V(ITERS, width, 4, L),
            V(2, SUB, L), V(2, SUB, L),
            V(ITERS, 2, SUB, LANES), V(ITERS, 3, SUB, LANES), V(ITERS, nlon, SUB, LANES),
            V(ITERS, 2, LANES), V(ITERS, n, 2, LANES), V(9, L // LANES, ncols, LANES), V(nlon, R, SUB, LANES),
            V(4, SUB, L), V(2, SUB, L), V(3, ncols, nrows), V(3, ncols, nrows), V(ncols, nrows),
            pltpu.VMEM((ncols, nrows), jnp.int32), pltpu.VMEM((ncols, nrows), jnp.int32), S(5),
            S(ITERS, 2), S(ITERS, 2), S(2), S(2), S(ITERS, 3), S(ITERS, 3), S(ITERS, nlon), S(ITERS, nlon),
            S(ITERS, n), S(ITERS, n),
        ],
        compiler_params=pltpu.CompilerParams(
            collective_id=0, has_side_effects=True, vmem_limit_bytes=67043328 - 1024 * 1024
        ),
    )(kernel_weights, fold_partner, strain_rate, stress_start, concentration, cell_class, land_mask)
    return stress, damage, mean


def solution(mesh):
    in_specs = (
        P(None, "lon", "lat"),
        P(None, "lon", "lat"),
        P("lon", "lat"),
        P(("member", "lon"), "lat"),
        P("lon", "lat"),
        P(),
        P(),
    )
    out_specs = (P(None, ("member", "lon"), "lat"), P(("member", "lon"), "lat"), P("member"))
    body = functools.partial(shards, mesh.shape["lon"], mesh.shape["lat"])
    return jax.shard_map(body, mesh=mesh, in_specs=in_specs, out_specs=out_specs, check_vma=False)
```
